8 devices in a mesh: ez: 2 (over z, y), ey: 2 (over x), ex: 2 (over core).
Axes of the slice: x: 2, y: 2, z: 1, core: 2. Of those that a mesh axis runs over, the one named last changes fastest.
Arguments:
- tokens: bfloat16 [2048, 1024], P(('ez', 'ey', 'ex'))
- expert_ids: int32 [2048, 8], P(('ez', 'ey', 'ex'))
- gate_weights: float32 [2048, 8], P(('ez', 'ey', 'ex'))
- w_gate: bfloat16 [32, 1024, 512], P(('ez', 'ey', 'ex'))
- w_up: bfloat16 [32, 1024, 512], P(('ez', 'ey', 'ex'))
- w_down: bfloat16 [32, 512, 1024], P(('ez', 'ey', 'ex'))
Outputs:
- output: bfloat16 [2048, 1024], P(('ez', 'ey', 'ex'))
All inputs are finite; a program needn't handle non-finite values.
Results may differ from the reference program's by a relative error of at most 0.00588897.
Values are sent between devices in bfloat16 or wider.
A program may use at most 1 GiB of HBM per device.

```python
import jax
import jax.numpy as jnp
from jax import lax

HIDDEN = 1024
EXPERT_FF = 512
EXPERTS = 32
TOP_K = 8
TOKENS = 256
DEVICES = 8
TOTAL_TOK = DEVICES * TOKENS
LOCAL_EXPERTS = EXPERTS // DEVICES
PER_EXPERT = TOTAL_TOK * TOP_K // EXPERTS


def draw_routing(route_key):
    def one_source(src_key):
        key_first, key_rest, key_dev, key_order = jax.random.split(src_key, 4)
        first_block = jax.random.permutation(key_first, LOCAL_EXPERTS)
        rest_block = jax.random.permutation(key_rest, EXPERTS - LOCAL_EXPERTS) + LOCAL_EXPERTS
        positions = jnp.arange(EXPERTS)
        spaced = positions % DEVICES == 0
        first_idx = jnp.clip(positions // DEVICES, 0, LOCAL_EXPERTS - 1)
        rest_idx = jnp.clip(positions - positions // DEVICES - 1, 0, EXPERTS - LOCAL_EXPERTS - 1)
        expert_cycle = jnp.where(spaced, first_block[first_idx], rest_block[rest_idx])
        dev_perm = jax.random.permutation(key_dev, DEVICES)
        expert_cycle = dev_perm[expert_cycle // LOCAL_EXPERTS] * LOCAL_EXPERTS + expert_cycle % LOCAL_EXPERTS
        tok_perm = jax.random.permutation(key_order, TOKENS)
        slot_pos = tok_perm[:, None] * TOP_K + jnp.arange(TOP_K)[None, :]
        return expert_cycle[slot_pos % EXPERTS]
    src_keys = jax.random.split(route_key, DEVICES)
    return jax.vmap(one_source)(src_keys).reshape(TOTAL_TOK, TOP_K).astype(jnp.int32)


def setup_inputs(seed: int = 0) -> dict:
    root_key = jax.random.key(seed)
    key_tok, key_ids, key_gate, key_w1, key_w3, key_w2 = jax.random.split(root_key, 6)
    tokens = jax.random.normal(key_tok, (TOTAL_TOK, HIDDEN), jnp.float32).astype(jnp.bfloat16)
    expert_ids = draw_routing(key_ids)
    gate_logits = 0.7 * jax.random.normal(key_gate, (TOTAL_TOK, TOP_K), jnp.float32)
    gate_weights = jax.nn.softmax(gate_logits, axis=-1)
    w_gate = (jax.random.normal(key_w1, (EXPERTS, HIDDEN, EXPERT_FF), jnp.float32) * HIDDEN ** -0.5).astype(jnp.bfloat16)
    w_up = (jax.random.normal(key_w3, (EXPERTS, HIDDEN, EXPERT_FF), jnp.float32) * HIDDEN ** -0.5).astype(jnp.bfloat16)
    w_down = (jax.random.normal(key_w2, (EXPERTS, EXPERT_FF, HIDDEN), jnp.float32) * (2.0 * EXPERT_FF ** -0.5)).astype(jnp.bfloat16)
    return {"tokens": tokens, "expert_ids": expert_ids, "gate_weights": gate_weights, "w_gate": w_gate, "w_up": w_up, "w_down": w_down}


def reference(tokens, expert_ids, gate_weights, w_gate, w_up, w_down):
    sort_order = jnp.argsort(expert_ids.reshape(-1), stable=True)
    rows_by_expert = (sort_order // TOP_K).reshape(EXPERTS, PER_EXPERT)
    gates_by_expert = gate_weights.reshape(-1)[sort_order].reshape(EXPERTS, PER_EXPERT)

    def expert_step(acc_out, expert_args):
        row_ids, row_gates, gate_mat, up_mat, down_mat = expert_args
        x_rows = tokens[row_ids]
        gate_act = jnp.dot(x_rows, gate_mat, preferred_element_type=jnp.float32)
        up_act = jnp.dot(x_rows, up_mat, preferred_element_type=jnp.float32)
        hidden_act = (jax.nn.silu(gate_act) * up_act).astype(jnp.bfloat16)
        expert_out = jnp.dot(hidden_act, down_mat, preferred_element_type=jnp.float32)
        acc_out = acc_out.at[row_ids].add(expert_out * row_gates[:, None])
        return acc_out, None

    init_acc = jnp.zeros((TOTAL_TOK, HIDDEN), jnp.float32)
    moe_sum = lax.scan(expert_step, init_acc, (rows_by_expert, gates_by_expert, w_gate, w_up, w_down))[0]
    return (tokens.astype(jnp.float32) + moe_sum).astype(jnp.bfloat16)
```

```python
import functools

import jax
import jax.numpy as jnp
from jax import lax
from jax.experimental import pallas as pl
from jax.experimental.pallas import tpu as pltpu
from jax.sharding import PartitionSpec as P

MESH = pl.DeviceIdType.MESH
F32, BF16 = jnp.float32, jnp.bfloat16

BLOCKS = (
    ((0, 0), (0, 1)),
    ((1, 0), (1, 1)),
    ((3, 0), (5, 1)),
    ((2, 0), (4, 1)),
    ((7, 0), (7, 1)),
    ((6, 0), (6, 1)),
    ((3, 1), (5, 0)),
    ((2, 1), (4, 0)),
)
GATE_ORDER = (0, 1, 4, 5, 2, 3, 6, 7)


def moe_kernel(
    x_hbm, ids_hbm, gates_hbm, w1_hbm, w3_hbm, w2_hbm, y_hbm,
    xs, w1, w3, w2, ids, gates, gsend, g_a, g_b, g_d, g_c, G,
    acc, own, out_c, rec_c, pb, r_a, r_b, d_a, d_b, y_buf, lsem, ssem, rsem,
):
    z, y, x = lax.axis_index("ez"), lax.axis_index("ey"), lax.axis_index("ex")
    me = 4 * z + 2 * y + x
    dev = {"A": (z, 1 - y, x), "B": (1 - z, y, x), "C": (z, y, 1 - x)}
    half = 128
    local_experts, top_k = w1.shape[0], ids.shape[0]
    count = [0, 0]

    def local(src, dst):
        copy = pltpu.make_async_copy(src, dst, lsem.at[count[0]])
        count[0] += 1
        return copy

    def remote(src, dst, to):
        copy = pltpu.make_async_remote_copy(
            src_ref=src, dst_ref=dst, send_sem=ssem.at[count[1]], recv_sem=rsem.at[count[1]],
            device_id=dev[to], device_id_type=MESH,
        )
        count[1] += 1
        sent.append(copy)
        return copy

    sent = []
    lo, hi = pl.ds(0, half), pl.ds(half, half)

    load_ids, load_gates = local(ids_hbm, ids), local(gates_hbm, gates)
    load_x = local(x_hbm, xs.at[0])
    load_ids.start()
    load_gates.start()
    load_x.start()
    load_w = []
    for e in range(local_experts):
        trio = [local(s.at[e], d.at[e]) for s, d in ((w1_hbm, w1), (w3_hbm, w3), (w2_hbm, w2))]
        for copy in trio:
            copy.start()
        load_w.append(trio)

    barrier = pltpu.get_barrier_semaphore()
    for to in "ABC":
        pl.semaphore_signal(barrier, inc=1, device_id=dev[to], device_id_type=MESH)

    load_ids.wait()
    load_gates.wait()
    ids_v, gates_v = ids[...], gates[...]
    for p, k in enumerate(GATE_ORDER):
        first = (me ^ k) * local_experts
        for e in range(local_experts):
            row = jnp.sum(jnp.where(ids_v == first + e, gates_v, 0.0), axis=0, keepdims=True)
            gsend[p, pl.ds(2 * e, 1), :] = row[:, :half]
            gsend[p, pl.ds(2 * e + 1, 1), :] = row[:, half:]
    load_x.wait()
    pl.semaphore_wait(barrier, 3)

    quarter = half // 2
    ag_a1 = remote(xs.at[0, lo], xs.at[3, lo], "A")
    ag_b1 = remote(xs.at[0, hi], xs.at[3, hi], "B")
    gs_a = remote(gsend.at[pl.ds(4, 4)], g_a, "A")
    gs_b = remote(gsend.at[pl.ds(2, 2)], g_b, "B")
    ag_c1 = remote(xs.at[0], xs.at[1], "C")
    gs_c = remote(gsend.at[pl.ds(1, 1)], g_c.at[pl.ds(0, 1)], "C")
    ag_a2 = [remote(xs.at[0, pl.ds(half + q * quarter, quarter)], xs.at[7, pl.ds(q * quarter, quarter)], "A") for q in range(2)]
    ag_b2 = [remote(xs.at[0, pl.ds(q * quarter, quarter)], xs.at[7, pl.ds(half + q * quarter, quarter)], "B") for q in range(2)]
    fw_a = remote(xs.at[3, hi], xs.at[5, hi], "A")
    fw_b = remote(xs.at[3, lo], xs.at[5, lo], "B")
    gf_b = remote(g_a.at[pl.ds(2, 2)], g_d, "B")
    d2d_3 = remote(xs.at[3], xs.at[2], "C")
    d2d_5 = remote(xs.at[5], xs.at[4], "C")
    d2d_7 = remote(xs.at[7], xs.at[6], "C")
    gc_3 = remote(g_a.at[pl.ds(1, 1)], g_c.at[pl.ds(1, 1)], "C")
    gc_5 = remote(g_b.at[pl.ds(1, 1)], g_c.at[pl.ds(2, 1)], "C")
    gc_7 = remote(g_d.at[pl.ds(1, 1)], g_c.at[pl.ds(3, 1)], "C")

    for copy in (ag_a1, ag_b1, ag_c1, gs_c, gs_a, gs_b, ag_a2[0], ag_b2[0]):
        copy.start()

    def forward_3():
        ag_a1.wait_recv()
        ag_b1.wait_recv()
        gs_a.wait_recv()
        gs_b.wait_recv()
        for copy in (fw_a, fw_b, gf_b, d2d_3, gc_3, gc_5, ag_a2[1], ag_b2[1]):
            copy.start()

    def forward_5():
        fw_a.wait_recv()
        fw_b.wait_recv()
        gf_b.wait_recv()
        d2d_5.start()
        gc_7.start()

    def forward_7():
        for copy in ag_a2 + ag_b2:
            copy.wait_recv()
        d2d_7.start()

    def gate_tile(owner):
        return {
            0: gsend.at[0], 1: g_c.at[0], 2: g_a.at[0], 3: g_c.at[1],
            4: g_b.at[0], 5: g_c.at[2], 6: g_d.at[0], 7: g_c.at[3],
        }[owner]

    def hidden(s, e):
        rows = xs[s]
        mask = jnp.concatenate([G[e]] * (w1.shape[2] // 128), axis=1) > 0.0
        a = jnp.dot(rows, w1[e], preferred_element_type=F32)
        b = jnp.dot(rows, w3[e], preferred_element_type=F32)
        return jnp.where(mask, a * (1.0 / (1.0 + jnp.exp(-a))) * b, 0.0).astype(BF16)

    def experts(s, total, hooks=None):
        hooks = hooks or {}
        for e in range(local_experts):
            for i, (owner, h) in enumerate(BLOCKS[s]):
                row = gate_tile(owner)[pl.ds(2 * e + h, 1), :]
                G[e, pl.ds(i * half, half), :] = jnp.broadcast_to(row, (half, half)).T
        act = None
        for e in range(local_experts + 1):
            if e in hooks:
                hooks[e]()
            later = hidden(s, e) if e < local_experts else None
            if act is not None:
                out = jnp.dot(act, w2[e - 1], preferred_element_type=F32)
                out = out * jnp.concatenate([G[e - 1]] * (w2.shape[2] // 128), axis=1)
                if e == 1:
                    total[...] = out
                else:
                    total[...] += out
            act = later

    def wait_weights(e):
        for copy in load_w[e]:
            copy.wait()

    experts(0, own, {e: functools.partial(wait_weights, e) for e in range(local_experts)})
    ag_c1.wait_recv()
    gs_c.wait_recv()
    experts(1, acc, {3: forward_3})
    out_c[0] = acc[...].astype(BF16)
    rs_c = [remote(out_c.at[i], rec_c.at[i], "C") for i in range(4)]
    rs_c[0].start()

    d2d_3.wait_recv()
    gc_3.wait_recv()
    gc_5.wait_recv()
    experts(2, acc)
    out_c[1] = acc[...].astype(BF16)
    rs_c[1].start()
    experts(3, acc, {3: forward_5})
    rs_c[1].wait_recv()
    pb[0] = (acc[...] + rec_c[1].astype(F32)).astype(BF16)
    rs_a1 = remote(pb.at[0, lo], r_a.at[lo], "A")
    rs_b1 = remote(pb.at[0, hi], r_b.at[hi], "B")
    rs_a1.start()
    rs_b1.start()

    d2d_5.wait_recv()
    gc_7.wait_recv()
    experts(4, acc)
    out_c[2] = acc[...].astype(BF16)
    rs_c[2].start()
    experts(5, acc, {2: forward_7})
    rs_c[2].wait_recv()
    pb[1] = (acc[...] + rec_c[2].astype(F32)).astype(BF16)
    rs_d = []
    for q in range(2):
        rs_d.append((
            remote(pb.at[1, pl.ds(q * quarter, quarter)], d_a.at[pl.ds(q * quarter, quarter)], "A"),
            remote(pb.at[1, pl.ds(half + q * quarter, quarter)], d_b.at[pl.ds(q * quarter, quarter)], "B"),
        ))
        for copy in rs_d[q]:
            copy.start()

    d2d_7.wait_recv()
    experts(6, acc)
    out_c[3] = acc[...].astype(BF16)
    rs_c[3].start()
    experts(7, acc)
    rs_c[3].wait_recv()
    rs_2 = []
    for q in range(2):
        upper, lower = pl.ds(q * quarter, quarter), pl.ds(half + q * quarter, quarter)
        rs_d[q][1].wait_recv()
        pb[2, upper] = (acc[upper, :] + rec_c[3, upper].astype(F32) + d_b[upper].astype(F32)).astype(BF16)
        rs_2.append([remote(pb.at[2, upper], r_a.at[lower], "A")])
        rs_2[q][0].start()
        rs_d[q][0].wait_recv()
        pb[2, lower] = (acc[lower, :] + rec_c[3, lower].astype(F32) + d_a[upper].astype(F32)).astype(BF16)
        rs_2[q].append(remote(pb.at[2, lower], r_b.at[upper], "B"))
        rs_2[q][1].start()

    rs_c[0].wait_recv()
    rs_a1.wait_recv()
    rs_b1.wait_recv()
    own[...] = own[...] + rec_c[0].astype(F32) + xs[0].astype(F32)
    own[lo, :] = own[lo, :] + r_a[lo].astype(F32)
    own[hi, :] = own[hi, :] + r_b[hi].astype(F32)
    stores = []
    for q in range(2):
        upper, lower = pl.ds(q * quarter, quarter), pl.ds(half + q * quarter, quarter)
        rs_2[q][0].wait_recv()
        y_buf[lower] = (own[lower, :] + r_a[lower].astype(F32)).astype(BF16)
        rs_2[q][1].wait_recv()
        y_buf[upper] = (own[upper, :] + r_b[upper].astype(F32)).astype(BF16)
        for rows in (upper, lower):
            stores.append(local(y_buf.at[rows], y_hbm.at[rows]))
            stores[-1].start()
    for copy in stores:
        copy.wait()
    for copy in sent:
        copy.wait_send()


def solution(mesh):
    axes = tuple(mesh.axis_names)
    row_spec, w_spec = P(axes, None), P(axes, None, None)

    def local_layer(tokens, expert_ids, gate_weights, w_gate, w_up, w_down):
        rows, width = tokens.shape
        experts, _, ff = w_gate.shape
        top_k = expert_ids.shape[1]
        any_space = pl.BlockSpec(memory_space=pl.ANY)
        return pl.pallas_call(
            moe_kernel,
            name="moe_layer",
            out_shape=jax.ShapeDtypeStruct((rows, width), BF16),
            in_specs=[any_space] * 6,
            out_specs=any_space,
            scratch_shapes=[
                pltpu.VMEM((8, rows, width), BF16),
                pltpu.VMEM((experts, width, ff), BF16),
                pltpu.VMEM((experts, width, ff), BF16),
                pltpu.VMEM((experts, ff, width), BF16),
                pltpu.VMEM((top_k, rows), jnp.int32),
                pltpu.VMEM((top_k, rows), F32),
                pltpu.VMEM((8, 8, 128), F32),
                pltpu.VMEM((4, 8, 128), F32),
                pltpu.VMEM((2, 8, 128), F32),
                pltpu.VMEM((2, 8, 128), F32),
                pltpu.VMEM((4, 8, 128), F32),
                pltpu.VMEM((experts, rows, 128), F32),
                pltpu.VMEM((rows, width), F32),
                pltpu.VMEM((rows, width), F32),
                pltpu.VMEM((4, rows, width), BF16),
                pltpu.VMEM((4, rows, width), BF16),
                pltpu.VMEM((3, rows, width), BF16),
                pltpu.VMEM((rows, width), BF16),
                pltpu.VMEM((rows, width), BF16),
                pltpu.VMEM((rows // 2, width), BF16),
                pltpu.VMEM((rows // 2, width), BF16),
                pltpu.VMEM((rows, width), BF16),
                pltpu.SemaphoreType.DMA((20,)),
                pltpu.SemaphoreType.DMA((40,)),
                pltpu.SemaphoreType.DMA((40,)),
            ],
            compiler_params=pltpu.CompilerParams(
                collective_id=0, has_side_effects=True, vmem_limit_bytes=60 * 2**20
            ),
        )(tokens, expert_ids.T, gate_weights.T, w_gate, w_up, w_down)

    return jax.shard_map(
        local_layer, mesh=mesh,
        in_specs=(row_spec, row_spec, row_spec, w_spec, w_spec, w_spec),
        out_specs=row_spec, check_vma=False,
    )
```

```python
import functools

import jax
import jax.numpy as jnp
from jax import lax
from jax.experimental import pallas as pl
from jax.experimental.pallas import tpu as pltpu
from jax.sharding import PartitionSpec as P

MESH = pl.DeviceIdType.MESH
F32, BF16 = jnp.float32, jnp.bfloat16

BLOCKS = (
    ((0, 0, 0), (0, 0, 1), (0, 1, 0), (0, 1, 1)),
    ((1, 0, 0), (1, 0, 1), (1, 1, 0), (1, 1, 1)),
    ((3, 0, 0), (5, 1, 1), (2, 0, 0), (4, 1, 1)),
    ((5, 1, 0), (3, 0, 1), (4, 1, 0), (2, 0, 1)),
    ((7, 0, 0), (7, 1, 1), (6, 0, 0), (6, 1, 1)),
    ((7, 1, 0), (7, 0, 1), (6, 1, 0), (6, 0, 1)),
    ((5, 0, 0), (3, 1, 1), (4, 0, 0), (2, 1, 1)),
    ((3, 1, 0), (5, 0, 1), (2, 1, 0), (4, 0, 1)),
)
GATE_ORDER = (0, 1, 4, 5, 2, 3, 6, 7)
QUARTER = 64


def place(piece):
    for s, pieces in enumerate(BLOCKS):
        if piece in pieces:
            return s, pieces.index(piece) * QUARTER


def token_row(half, quarter):
    return (2 * half + quarter) * QUARTER


def moe_kernel(
    x_hbm, ids_hbm, gates_hbm, w1_hbm, w3_hbm, w2_hbm, y_hbm,
    xs, w1, w3, w2, ids, gates, gsend, g_a, g_b, g_d, g_c, G,
    acc, own, out_c1, rec_c1, out_c, rec_c, pb, r_a, r_b, d_a, d_b, y_buf, lsem, ssem, rsem,
):
    z, y, x = lax.axis_index("ez"), lax.axis_index("ey"), lax.axis_index("ex")
    me = 4 * z + 2 * y + x
    dev = {"A": (z, 1 - y, x), "B": (1 - z, y, x), "C": (z, y, 1 - x)}
    half = 2 * QUARTER
    local_experts = w1.shape[0]
    count = [0, 0]
    sent = []

    def local(src, dst):
        copy = pltpu.make_async_copy(src, dst, lsem.at[count[0]])
        count[0] += 1
        return copy

    def remote(src, dst, to):
        copy = pltpu.make_async_remote_copy(
            src_ref=src, dst_ref=dst, send_sem=ssem.at[count[1]], recv_sem=rsem.at[count[1]],
            device_id=dev[to], device_id_type=MESH,
        )
        count[1] += 1
        sent.append(copy)
        return copy

    def rows(piece, skip=0, size=QUARTER):
        s, row = place(piece)
        return xs.at[s, pl.ds(row + skip, size)]

    def start(copies):
        for copy in copies:
            copy.start()

    def arrive(copies):
        for copy in copies:
            copy.wait_recv()

    load_x = local(x_hbm, xs.at[0])
    load_ids, load_gates = local(ids_hbm, ids), local(gates_hbm, gates)
    start((load_x, load_ids, load_gates))
    load_w = []
    for e in range(local_experts):
        load_w.append([local(s.at[e], d.at[e]) for s, d in ((w1_hbm, w1), (w3_hbm, w3), (w2_hbm, w2))])
        start(load_w[e])
    load_w.append([])

    barrier = pltpu.get_barrier_semaphore()
    for to in "ABC":
        pl.semaphore_signal(barrier, inc=1, device_id=dev[to], device_id_type=MESH)

    first, second, onward = ([], []), ([], []), ([], [])
    for i in range(2):
        s1, s2, s3 = 2 + i, 4 + i, 6 + i
        for owner, h, q in BLOCKS[s1][2:]:
            to, across = ("A", "B") if owner == 2 else ("B", "A")
            first[i].append(remote(rows((0, h, q)), rows((owner, h, q)), to))
            onward[i].append(remote(rows((owner, h, q)), rows((6, h, q)), across))
        for owner, h, q in BLOCKS[s3][2:]:
            to = "A" if owner == 2 else "B"
            cuts = ((0, 32), (32, 32)) if i == 0 else ((0, QUARTER),)
            second[i].append([remote(rows((0, h, q), *cut), rows((owner, h, q), *cut), to) for cut in cuts])
    core_own = remote(xs.at[0], xs.at[1], "C")
    upper, lower = pl.ds(0, half), pl.ds(half, half)
    core = {s: remote(xs.at[s, lower], xs.at[s, upper], "C") for s in range(2, 8)}
    gate_a = remote(gsend.at[pl.ds(4, 4)], g_a, "A")
    gate_b = remote(gsend.at[pl.ds(2, 2)], g_b, "B")
    gate_c = remote(gsend.at[pl.ds(1, 1)], g_c.at[pl.ds(0, 1)], "C")
    gate_d = remote(g_a.at[pl.ds(2, 2)], g_d, "B")
    gate_c3 = remote(g_a.at[pl.ds(1, 1)], g_c.at[pl.ds(1, 1)], "C")
    gate_c5 = remote(g_b.at[pl.ds(1, 1)], g_c.at[pl.ds(2, 1)], "C")
    gate_c7 = remote(g_d.at[pl.ds(1, 1)], g_c.at[pl.ds(3, 1)], "C")

    load_x.wait()
    pl.semaphore_wait(barrier, 3)
    start(first[0])

    load_ids.wait()
    load_gates.wait()
    ids_v, gates_v = ids[...], gates[...]
    for p, k in enumerate(GATE_ORDER):
        base = (me ^ k) * local_experts
        for e in range(local_experts):
            row = jnp.sum(jnp.where(ids_v == base + e, gates_v, 0.0), axis=0, keepdims=True)
            gsend[p, pl.ds(2 * e, 1), :] = row[:, :half]
            gsend[p, pl.ds(2 * e + 1, 1), :] = row[:, half:]
    start((gate_a, gate_b, gate_c, core_own))
    start(first[1])
    start([pieces[0] for pieces in second[0]])

    def pass_first_0():
        arrive(first[0])
        start(onward[0])
        core[2].start()
        arrive((gate_a, gate_b))
        start((gate_c3, gate_c5, gate_d))

    def pass_first_1():
        arrive(first[1])
        start(onward[1])
        core[3].start()
        start([pieces[1] for pieces in second[0]])
        start([pieces[0] for pieces in second[1]])

    def pass_diagonal_0():
        arrive(onward[0])
        core[4].start()
        gate_d.wait_recv()
        gate_c7.start()

    def pass_diagonal_1():
        arrive(onward[1])
        core[5].start()

    def pass_second(i):
        for pieces in second[i]:
            arrive(pieces)
        core[6 + i].start()

    gate_tiles = {
        0: gsend.at[0], 1: g_c.at[0], 2: g_a.at[0], 3: g_c.at[1],
        4: g_b.at[0], 5: g_c.at[2], 6: g_d.at[0], 7: g_c.at[3],
    }

    def hidden(s, part, e):
        tokens = xs[s, part]
        mask = jnp.concatenate([G[e, part]] * (w1.shape[2] // 128), axis=1) > 0.0
        a = jnp.dot(tokens, w1[e], preferred_element_type=F32)
        b = jnp.dot(tokens, w3[e], preferred_element_type=F32)
        return jnp.where(mask, a * (1.0 / (1.0 + jnp.exp(-a))) * b, 0.0).astype(BF16)

    def experts(s, total, finish, hooks=None, parts=(0, 1)):
        hooks = hooks or {}
        part = pl.ds(parts[0] * half, len(parts) * half)
        left = lax.broadcasted_iota(jnp.int32, (1, half), 1) < QUARTER
        for e in range(local_experts):
            for i in parts:
                (o0, h0, _), (o1, h1, _) = BLOCKS[s][2 * i:2 * i + 2]
                row = gate_tiles[o0][pl.ds(2 * e + h0, 1), :]
                if (o0, h0) != (o1, h1):
                    row = jnp.where(left, row, gate_tiles[o1][pl.ds(2 * e + h1, 1), :])
                G[e, pl.ds(i * half, half), :] = jnp.broadcast_to(row, (half, half)).T
        act = None
        for e in range(local_experts + 1):
            for hook in hooks.get(e, ()):
                hook()
            later = hidden(s, part, e) if e < local_experts else None
            if act is not None:
                out = jnp.dot(act, w2[e - 1], preferred_element_type=F32)
                out = out * jnp.concatenate([G[e - 1, part]] * (w2.shape[2] // 128), axis=1)
                if e == 1:
                    total[part, :] = out
                elif e < local_experts:
                    total[part, :] += out
                else:
                    finish(out)
            act = later

    back_c = {s: remote(out_c.at[s - 2], rec_c.at[s - 2], "C") for s in range(2, 8)}
    back_own = [remote(out_c1.at[part], rec_c1.at[part], "C") for part in (upper, lower)]
    back, through = {}, {}

    def finish_own(out):
        own[...] = own[...] + out

    def finish_core_own(i):
        part = (upper, lower)[i]

        def finish(out):
            out_c1[part, :] = (acc[0, part, :] + out).astype(BF16)
        return finish

    def finish_pair(s):
        def finish(out):
            out_c[s - 2] = (acc[s % 2, upper, :] + out[:half]).astype(BF16)
            acc[s % 2, lower, :] += out[half:]
        return finish

    def send_chip(s):
        i = s - 2
        back_c[s].wait_recv()
        for j, (owner, h, q) in enumerate(BLOCKS[s][2:]):
            part = pl.ds(j * QUARTER, QUARTER)
            total = acc[s % 2, pl.ds(half + j * QUARTER, QUARTER), :] + rec_c[i, part, :].astype(F32)
            if (owner, h) in ((2, 1), (4, 0)):
                through[6, h, q].wait_recv()
                total = total + (d_b if owner == 2 else d_a)[q].astype(F32)
            pb[i, part, :] = total.astype(BF16)
            row = pl.ds(token_row(h, q), QUARTER)
            if owner == 6:
                to, dst = ("A", d_a.at[q]) if h == 0 else ("B", d_b.at[q])
                through[6, h, q] = copy = remote(pb.at[i, part], dst, to)
            else:
                to, dst = ("A", r_a.at[row]) if owner == 2 else ("B", r_b.at[row])
                back[owner, h, q] = copy = remote(pb.at[i, part], dst, to)
            copy.start()

    def pair(s, hooks):
        core[s].wait_recv()
        experts(s, acc.at[s % 2], finish_pair(s), hooks)
        back_c[s].start()

    def await_weights(e):
        for copy in load_w[e - 1][2:] + load_w[e][:2]:
            copy.wait()

    do = functools.partial
    experts(0, own, finish_own, {e: [do(await_weights, e)] for e in range(local_experts + 1)})
    pass_first_0()
    arrive((core_own, gate_c))
    experts(1, acc.at[0], finish_core_own(0), parts=(0,))
    back_own[0].start()
    arrive((gate_c3, gate_c5))
    pair(2, {2: [pass_first_1]})
    pair(3, {3: [do(send_chip, 2), pass_diagonal_0]})
    gate_c7.wait_recv()
    pair(4, {3: [do(send_chip, 3), pass_diagonal_1]})
    pair(5, {3: [do(send_chip, 4), do(pass_second, 0), do(pass_second, 1)]})
    pair(6, {3: [do(send_chip, 5)]})
    pair(7, {3: [do(send_chip, 6)]})
    experts(1, acc.at[0], finish_core_own(1), {3: [do(send_chip, 7)]}, parts=(1,))
    back_own[1].start()

    arrive(back_own)
    own[...] = own[...] + rec_c1[...].astype(F32) + xs[0].astype(F32)
    for q in range(2):
        row_0, row_1 = pl.ds(token_row(0, q), QUARTER), pl.ds(token_row(1, q), QUARTER)
        arrive((back[2, 0, q], back[4, 1, q]))
        own[row_0, :] = own[row_0, :] + r_a[row_0, :].astype(F32)
        own[row_1, :] = own[row_1, :] + r_b[row_1, :].astype(F32)
    stores = []
    for s in (6, 7):
        for owner, h, q in BLOCKS[s][2:]:
            row = pl.ds(token_row(h, q), QUARTER)
            back[owner, h, q].wait_recv()
            y_buf[row, :] = (own[row, :] + (r_a if owner == 2 else r_b)[row, :].astype(F32)).astype(BF16)
            stores.append(local(y_buf.at[row], y_hbm.at[row]))
            stores[-1].start()
    for copy in stores:
        copy.wait()
    for copy in sent:
        copy.wait_send()


def solution(mesh):
    axes = tuple(mesh.axis_names)
    row_spec, w_spec = P(axes, None), P(axes, None, None)

    def local_layer(tokens, expert_ids, gate_weights, w_gate, w_up, w_down):
        rows, width = tokens.shape
        experts, _, ff = w_gate.shape
        top_k = expert_ids.shape[1]
        return pl.pallas_call(
            moe_kernel,
            name="moe_layer",
            out_shape=jax.ShapeDtypeStruct((rows, width), BF16),
            in_specs=[pl.BlockSpec(memory_space=pltpu.HBM)] * 6,
            out_specs=pl.BlockSpec(memory_space=pltpu.HBM),
            scratch_shapes=[
                pltpu.VMEM((8, rows, width), BF16),
                pltpu.VMEM((experts, width, ff), BF16),
                pltpu.VMEM((experts, width, ff), BF16),
                pltpu.VMEM((experts, ff, width), BF16),
                pltpu.VMEM((top_k, rows), jnp.int32),
                pltpu.VMEM((top_k, rows), F32),
                pltpu.VMEM((8, 8, 128), F32),
                pltpu.VMEM((4, 8, 128), F32),
                pltpu.VMEM((2, 8, 128), F32),
                pltpu.VMEM((2, 8, 128), F32),
                pltpu.VMEM((4, 8, 128), F32),
                pltpu.VMEM((experts, rows, 128), F32),
                pltpu.VMEM((2, rows, width), F32),
                pltpu.VMEM((rows, width), F32),
                pltpu.VMEM((rows, width), BF16),
                pltpu.VMEM((rows, width), BF16),
                pltpu.VMEM((6, rows // 2, width), BF16),
                pltpu.VMEM((6, rows // 2, width), BF16),
                pltpu.VMEM((6, rows // 2, width), BF16),
                pltpu.VMEM((rows, width), BF16),
                pltpu.VMEM((rows, width), BF16),
                pltpu.VMEM((2, QUARTER, width), BF16),
                pltpu.VMEM((2, QUARTER, width), BF16),
                pltpu.VMEM((rows, width), BF16),
                pltpu.SemaphoreType.DMA((20,)),
                pltpu.SemaphoreType.DMA((48,)),
                pltpu.SemaphoreType.DMA((48,)),
            ],
            compiler_params=pltpu.CompilerParams(
                collective_id=0, has_side_effects=True, vmem_limit_bytes=60 * 2**20
            ),
        )(tokens, expert_ids.T, gate_weights.T, w_gate, w_up, w_down)

    return jax.shard_map(
        local_layer, mesh=mesh,
        in_specs=(row_spec, row_spec, row_spec, w_spec, w_spec, w_spec),
        out_specs=row_spec, check_vma=False,
    )
```

```python
import functools

import jax
import jax.numpy as jnp
from jax import lax
from jax.experimental import pallas as pl
from jax.experimental.pallas import tpu as pltpu
from jax.sharding import PartitionSpec as P

MESH = pl.DeviceIdType.MESH
F32, BF16 = jnp.float32, jnp.bfloat16

BLOCKS = (
    ((0, 0, 0), (0, 0, 1), (0, 1, 0), (0, 1, 1)),
    ((1, 0, 0), (1, 0, 1), (1, 1, 0), (1, 1, 1)),
    ((3, 0, 0), (5, 1, 1), (2, 0, 0), (4, 1, 1)),
    ((5, 1, 0), (3, 0, 1), (4, 1, 0), (2, 0, 1)),
    ((7, 0, 0), (7, 1, 1), (6, 0, 0), (6, 1, 1)),
    ((7, 1, 0), (7, 0, 1), (6, 1, 0), (6, 0, 1)),
    ((5, 0, 0), (3, 1, 1), (4, 0, 0), (2, 1, 1)),
    ((3, 1, 0), (5, 0, 1), (2, 1, 0), (4, 0, 1)),
)
GATE_ORDER = (0, 1, 4, 5, 2, 3, 6, 7)
QUARTER = 64


def place(piece):
    for s, pieces in enumerate(BLOCKS):
        if piece in pieces:
            return s, pieces.index(piece) * QUARTER


def token_row(half, quarter):
    return (2 * half + quarter) * QUARTER


def moe_kernel(
    x_hbm, ids_hbm, gates_hbm, w1_hbm, w3_hbm, w2_hbm, y_ref,
    xs, w1, w3, w2, ids, gates, gsend, g_a, g_b, g_d, g_c, G,
    acc, own, out_c1, rec_c1, out_c, rec_c, pb, r_a, r_b, d_ab, lsem, ssem, rsem,
):
    z, y, x = lax.axis_index("ez"), lax.axis_index("ey"), lax.axis_index("ex")
    me = 4 * z + 2 * y + x
    dev = {"A": (z, 1 - y, x), "B": (1 - z, y, x), "C": (z, y, 1 - x)}
    half = 2 * QUARTER
    local_experts = w1.shape[0]
    names = {}

    def await_all(sem, like):
        pltpu.make_async_copy(like, like, sem).wait()

    def received(name):
        return rsem.at[names.setdefault(name, len(names))]

    def remote(src, dst, to, name, kind=0):
        return pltpu.make_async_remote_copy(
            src_ref=src, dst_ref=dst, send_sem=ssem.at[kind], recv_sem=received(name),
            device_id=dev[to], device_id_type=MESH,
        )

    def rows(piece, skip=0, size=QUARTER):
        s, row = place(piece)
        return xs.at[s, pl.ds(row + skip, size)]

    def start(copies):
        for copy in copies:
            copy.start()

    def arrive(name, like):
        await_all(received(name), like)

    def load(src, dst, sem):
        pltpu.make_async_copy(src, dst, lsem.at[sem]).start()

    load(x_hbm, xs.at[0], 0)
    load(ids_hbm, ids, 1)
    load(gates_hbm, gates, 1)
    for e in range(local_experts):
        load(w1_hbm.at[e], w1.at[e], 2 + e)
        load(w3_hbm.at[e], w3.at[e], 2 + e)
        load(w2_hbm.at[e], w2.at[e], 3 + e)

    def await_weights(e):
        matrices = 2 * (e < local_experts) + (e > 0)
        await_all(lsem.at[2 + e], w1.at[pl.ds(0, matrices)])

    barrier = pltpu.get_barrier_semaphore()
    for to in "ABC":
        pl.semaphore_signal(barrier, inc=1, device_id=dev[to], device_id_type=MESH)

    first, second, onward = ([], []), ([], []), ([], [])
    for i in range(2):
        s1, s3 = 2 + i, 6 + i
        for owner, h, q in BLOCKS[s1][2:]:
            to, across = ("A", "B") if owner == 2 else ("B", "A")
            first[i].append(remote(rows((0, h, q)), rows((owner, h, q)), to, ("first", i)))
            onward[i].append(remote(rows((owner, h, q)), rows((6, h, q)), across, ("onward", i)))
        for owner, h, q in BLOCKS[s3][2:]:
            to = "A" if owner == 2 else "B"
            cuts = ((0, 32), (32, 32)) if i == 0 else ((0, QUARTER),)
            second[i].append([remote(rows((0, h, q), *cut), rows((owner, h, q), *cut), to, ("second", i)) for cut in cuts])
    core_own = remote(xs.at[0], xs.at[1], "C", "core_own")
    upper, lower = pl.ds(0, half), pl.ds(half, half)
    core = {s: remote(xs.at[s, lower], xs.at[s, upper], "C", ("core", s)) for s in range(2, 8)}
    gate_a = remote(gsend.at[pl.ds(4, 4)], g_a, "A", "gate_ab", 2)
    gate_b = remote(gsend.at[pl.ds(2, 2)], g_b, "B", "gate_ab", 2)
    gate_c = remote(gsend.at[pl.ds(1, 1)], g_c.at[pl.ds(0, 1)], "C", "gate_c", 2)
    gate_d = remote(g_a.at[pl.ds(2, 2)], g_d, "B", "gate_d", 2)
    gate_c3 = remote(g_a.at[pl.ds(1, 1)], g_c.at[pl.ds(1, 1)], "C", "gate_c35", 2)
    gate_c5 = remote(g_b.at[pl.ds(1, 1)], g_c.at[pl.ds(2, 1)], "C", "gate_c35", 2)
    gate_c7 = remote(g_d.at[pl.ds(1, 1)], g_c.at[pl.ds(3, 1)], "C", "gate_c7", 2)

    await_all(lsem.at[0], xs.at[0])
    pl.semaphore_wait(barrier, 3)
    start(first[0])

    await_all(lsem.at[1], gsend.at[pl.ds(0, 4)])
    ids_v, gates_v = ids[...], gates[...]
    for p, k in enumerate(GATE_ORDER):
        base = (me ^ k) * local_experts
        for e in range(local_experts):
            row = jnp.sum(jnp.where(ids_v == base + e, gates_v, 0.0), axis=0, keepdims=True)
            gsend[p, pl.ds(2 * e, 1), :] = row[:, :half]
            gsend[p, pl.ds(2 * e + 1, 1), :] = row[:, half:]
    start((gate_a, gate_b, gate_c, core_own))
    start(first[1])
    start([pieces[0] for pieces in second[0]])

    def pass_first_0():
        arrive(("first", 0), xs.at[2, lower])
        start(onward[0])
        core[2].start()
        arrive("gate_ab", gsend.at[pl.ds(0, 6)])
        start((gate_c3, gate_c5, gate_d))

    def pass_first_1():
        arrive(("first", 1), xs.at[3, lower])
        start(onward[1])
        core[3].start()
        start([pieces[1] for pieces in second[0]])
        start([pieces[0] for pieces in second[1]])

    def pass_diagonal_0():
        arrive(("onward", 0), xs.at[4, lower])
        core[4].start()
        arrive("gate_d", g_d)
        gate_c7.start()

    def pass_diagonal_1():
        arrive(("onward", 1), xs.at[5, lower])
        core[5].start()

    def pass_second(i):
        arrive(("second", i), xs.at[6 + i, lower])
        core[6 + i].start()

    gate_tiles = {
        0: gsend.at[0], 1: g_c.at[0], 2: g_a.at[0], 3: g_c.at[1],
        4: g_b.at[0], 5: g_c.at[2], 6: g_d.at[0], 7: g_c.at[3],
    }

    def hidden(s, part, e):
        tokens = xs[s, part]
        mask = jnp.concatenate([G[e, part]] * (w1.shape[2] // 128), axis=1) > 0.0
        a = jnp.dot(tokens, w1[e], preferred_element_type=F32)
        b = jnp.dot(tokens, w3[e], preferred_element_type=F32)
        return jnp.where(mask, a * (1.0 / (1.0 + jnp.exp(-a))) * b, 0.0).astype(BF16)

    def experts(s, total, finish, hooks=None, parts=(0, 1)):
        hooks = hooks or {}
        part = pl.ds(parts[0] * half, len(parts) * half)
        left = lax.broadcasted_iota(jnp.int32, (1, half), 1) < QUARTER
        for e in range(local_experts):
            for i in parts:
                (o0, h0, _), (o1, h1, _) = BLOCKS[s][2 * i:2 * i + 2]
                row = gate_tiles[o0][pl.ds(2 * e + h0, 1), :]
                if (o0, h0) != (o1, h1):
                    row = jnp.where(left, row, gate_tiles[o1][pl.ds(2 * e + h1, 1), :])
                G[e, pl.ds(i * half, half), :] = jnp.broadcast_to(row, (half, half)).T
        act = None
        for e in range(local_experts + 1):
            for hook in hooks.get(e, ()):
                hook()
            later = hidden(s, part, e) if e < local_experts else None
            if act is not None:
                out = jnp.dot(act, w2[e - 1], preferred_element_type=F32)
                out = out * jnp.concatenate([G[e - 1, part]] * (w2.shape[2] // 128), axis=1)
                if e == 1:
                    total[part, :] = out
                elif e < local_experts:
                    total[part, :] += out
                else:
                    finish(out)
            act = later

    back_c = {s: remote(out_c.at[s - 2], rec_c.at[s - 2], "C", ("back_c", s), 1) for s in range(2, 8)}
    back_own = [remote(out_c1.at[part], rec_c1.at[part], "C", "back_own", 1) for part in (upper, lower)]

    def finish_own(out):
        own[...] = own[...] + out

    def finish_core_own(i):
        part = (upper, lower)[i]

        def finish(out):
            out_c1[part, :] = (acc[0, part, :] + out).astype(BF16)
        return finish

    def finish_pair(s):
        def finish(out):
            out_c[s - 2] = (acc[s % 2, upper, :] + out[:half]).astype(BF16)
            acc[s % 2, lower, :] += out[half:]
        return finish

    def send_chip(s):
        i = s - 2
        arrive(("back_c", s), rec_c.at[i])
        if s >= 6:
            arrive(("through", s - 2), d_ab.at[s - 6])
        for j, (owner, h, q) in enumerate(BLOCKS[s][2:]):
            part = pl.ds(j * QUARTER, QUARTER)
            total = acc[s % 2, pl.ds(half + j * QUARTER, QUARTER), :] + rec_c[i, part, :].astype(F32)
            if s >= 6:
                total = total + d_ab[s - 6, 1 if owner == 2 else 0].astype(F32)
            pb[i, part, :] = total.astype(BF16)
            row = pl.ds(token_row(h, q), QUARTER)
            if owner == 6:
                copy = remote(pb.at[i, part], d_ab.at[s - 4, h], "A" if h == 0 else "B", ("through", s), 1)
            else:
                name = ("back", s) if s >= 6 else "back"
                to, dst = ("A", r_a.at[row]) if owner == 2 else ("B", r_b.at[row])
                copy = remote(pb.at[i, part], dst, to, name, 1)
            copy.start()

    def pair(s, hooks):
        arrive(("core", s), xs.at[s, upper])
        experts(s, acc.at[s % 2], finish_pair(s), hooks)
        back_c[s].start()

    do = functools.partial
    experts(0, own, finish_own, {e: [do(await_weights, e)] for e in range(local_experts + 1)})
    pass_first_0()
    arrive("core_own", xs.at[1])
    arrive("gate_c", g_c.at[pl.ds(0, 1)])
    experts(1, acc.at[0], finish_core_own(0), parts=(0,))
    back_own[0].start()
    arrive("gate_c35", g_c.at[pl.ds(1, 2)])
    pair(2, {2: [pass_first_1]})
    pair(3, {3: [do(send_chip, 2), pass_diagonal_0]})
    arrive("gate_c7", g_c.at[pl.ds(3, 1)])
    pair(4, {3: [do(send_chip, 3), pass_diagonal_1]})
    pair(5, {3: [do(send_chip, 4), do(pass_second, 0), do(pass_second, 1)]})
    pair(6, {3: [do(send_chip, 5)]})
    pair(7, {2: [do(send_chip, 6)]})
    experts(1, acc.at[0], finish_core_own(1), {2: [do(send_chip, 7)]}, parts=(1,))
    back_own[1].start()

    arrive("back_own", rec_c1)
    own[...] = own[...] + rec_c1[...].astype(F32) + xs[0].astype(F32)
    arrive("back", r_a)
    own[upper, :] = own[upper, :] + r_a[upper, :].astype(F32)
    own[lower, :] = own[lower, :] + r_b[lower, :].astype(F32)
    for s in (6, 7):
        arrive(("back", s), r_a.at[upper])
        for owner, h, q in BLOCKS[s][2:]:
            row = pl.ds(token_row(h, q), QUARTER)
            y_ref[row, :] = (own[row, :] + (r_a if owner == 2 else r_b)[row, :].astype(F32)).astype(BF16)
    await_all(ssem.at[0], xs.at[pl.ds(0, 7)])
    await_all(ssem.at[1], xs.at[pl.ds(0, 7)])
    await_all(ssem.at[2], G.at[0, pl.ds(0, 96)])


def solution(mesh):
    axes = tuple(mesh.axis_names)
    row_spec, w_spec = P(axes, None), P(axes, None, None)

    def local_layer(tokens, expert_ids, gate_weights, w_gate, w_up, w_down):
        rows, width = tokens.shape
        experts, _, ff = w_gate.shape
        top_k = expert_ids.shape[1]
        return pl.pallas_call(
            moe_kernel,
            name="moe_layer",
            out_shape=jax.ShapeDtypeStruct((rows, width), BF16),
            in_specs=[pl.BlockSpec(memory_space=pltpu.HBM)] * 6,
            out_specs=pl.BlockSpec(memory_space=pltpu.VMEM),
            scratch_shapes=[
                pltpu.VMEM((8, rows, width), BF16),
                pltpu.VMEM((experts, width, ff), BF16),
                pltpu.VMEM((experts, width, ff), BF16),
                pltpu.VMEM((experts, ff, width), BF16),
                pltpu.VMEM((top_k, rows), jnp.int32),
                pltpu.VMEM((top_k, rows), F32),
                pltpu.VMEM((8, 8, 128), F32),
                pltpu.VMEM((4, 8, 128), F32),
                pltpu.VMEM((2, 8, 128), F32),
                pltpu.VMEM((2, 8, 128), F32),
                pltpu.VMEM((4, 8, 128), F32),
                pltpu.VMEM((experts, rows, 128), F32),
                pltpu.VMEM((2, rows, width), F32),
                pltpu.VMEM((rows, width), F32),
                pltpu.VMEM((rows, width), BF16),
                pltpu.VMEM((rows, width), BF16),
                pltpu.VMEM((6, rows // 2, width), BF16),
                pltpu.VMEM((6, rows // 2, width), BF16),
                pltpu.VMEM((6, rows // 2, width), BF16),
                pltpu.VMEM((rows, width), BF16),
                pltpu.VMEM((rows, width), BF16),
                pltpu.VMEM((2, 2, QUARTER, width), BF16),
                pltpu.SemaphoreType.DMA((7,)),
                pltpu.SemaphoreType.DMA((3,)),
                pltpu.SemaphoreType.DMA((30,)),
            ],
            compiler_params=pltpu.CompilerParams(
                collective_id=0, has_side_effects=True, vmem_limit_bytes=46 * 2**20
            ),
        )(*(pltpu.with_memory_space_constraint(v, pltpu.HBM) for v in (tokens, expert_ids.T, gate_weights.T, w_gate, w_up, w_down)))

    return jax.shard_map(
        local_layer, mesh=mesh,
        in_specs=(row_spec, row_spec, row_spec, w_spec, w_spec, w_spec),
        out_specs=row_spec, check_vma=False,
    )
```

```python
import functools

import jax
import jax.numpy as jnp
from jax import lax
from jax.experimental import pallas as pl
from jax.experimental.pallas import tpu as pltpu
from jax.sharding import PartitionSpec as P

MESH = pl.DeviceIdType.MESH
F32, BF16 = jnp.float32, jnp.bfloat16

BLOCKS = (
    ((0, 0, 0), (0, 0, 1), (0, 1, 0), (0, 1, 1)),
    ((1, 0, 0), (1, 0, 1), (1, 1, 0), (1, 1, 1)),
    ((3, 0, 0), (5, 1, 1), (2, 0, 0), (4, 1, 1)),
    ((5, 1, 0), (3, 0, 1), (4, 1, 0), (2, 0, 1)),
    ((7, 0, 0), (7, 1, 1), (6, 0, 0), (6, 1, 1)),
    ((7, 1, 0), (7, 0, 1), (6, 1, 0), (6, 0, 1)),
    ((5, 0, 0), (3, 1, 1), (4, 0, 0), (2, 1, 1)),
    ((3, 1, 0), (5, 0, 1), (2, 1, 0), (4, 0, 1)),
)
GATE_ORDER = (0, 1, 4, 5, 2, 3, 6, 7)
QUARTER = 64


def place(piece):
    for s, pieces in enumerate(BLOCKS):
        if piece in pieces:
            return s, pieces.index(piece) * QUARTER


def token_row(half, quarter):
    return (2 * half + quarter) * QUARTER


def moe_kernel(
    x_hbm, ids_hbm, gates_hbm, w1_hbm, w3_hbm, w2_hbm, y_ref,
    xs, w1, w3, w2, ids, gates, gsend, g_a, g_b, g_d, g_c, G,
    acc, own, out_c1, rec_c1, out_c, rec_c, pb, r_a, r_b, d_ab, lsem, ssem, rsem,
):
    z, y, x = lax.axis_index("ez"), lax.axis_index("ey"), lax.axis_index("ex")
    me = 4 * z + 2 * y + x
    dev = {"A": (z, 1 - y, x), "B": (1 - z, y, x), "C": (z, y, 1 - x)}
    half = 2 * QUARTER
    local_experts = w1.shape[0]
    names = {}

    def await_all(sem, like):
        pltpu.make_async_copy(like, like, sem).wait()

    def received(name):
        return rsem.at[names.setdefault(name, len(names))]

    def remote(src, dst, to, name, kind=0):
        return pltpu.make_async_remote_copy(
            src_ref=src, dst_ref=dst, send_sem=ssem.at[kind], recv_sem=received(name),
            device_id=dev[to], device_id_type=MESH,
        )

    def rows(piece, skip=0, size=QUARTER):
        s, row = place(piece)
        return xs.at[s, pl.ds(row + skip, size)]

    def start(copies):
        for copy in copies:
            copy.start()

    def arrive(name, like):
        await_all(received(name), like)

    def load(src, dst, sem):
        pltpu.make_async_copy(src, dst, lsem.at[sem]).start()

    load(ids_hbm, ids, 1)
    load(gates_hbm, gates, 1)
    load(x_hbm, xs.at[0], 0)
    for e in range(local_experts):
        load(w1_hbm.at[e], w1.at[e], 2 + e)
        load(w3_hbm.at[e], w3.at[e], 2 + e)
        load(w2_hbm.at[e], w2.at[e], 3 + e)

    def await_weights(e):
        matrices = 2 * (e < local_experts) + (e > 0)
        await_all(lsem.at[2 + e], w1.at[pl.ds(0, matrices)])

    barrier = pltpu.get_barrier_semaphore()
    for to in "ABC":
        pl.semaphore_signal(barrier, inc=1, device_id=dev[to], device_id_type=MESH)

    first, second, onward = ([], []), ([], []), ([], [])
    for i in range(2):
        s1, s3 = 2 + i, 6 + i
        for owner, h, q in BLOCKS[s1][2:]:
            to, across = ("A", "B") if owner == 2 else ("B", "A")
            first[i].append(remote(rows((0, h, q)), rows((owner, h, q)), to, ("first", i)))
            onward[i].append(remote(rows((owner, h, q)), rows((6, h, q)), across, ("onward", i)))
        for owner, h, q in BLOCKS[s3][2:]:
            to = "A" if owner == 2 else "B"
            cuts = ((0, 32), (32, 32)) if i == 0 else ((0, QUARTER),)
            second[i].append([remote(rows((0, h, q), *cut), rows((owner, h, q), *cut), to, "second") for cut in cuts])
    core_own = remote(xs.at[0], xs.at[1], "C", "core_own")
    upper, lower = pl.ds(0, half), pl.ds(half, half)
    core = {s: remote(xs.at[s, lower], xs.at[s, upper], "C", ("core", min(s, 6))) for s in range(2, 8)}
    gate_a = remote(gsend.at[pl.ds(4, 4)], g_a, "A", "gate_ab", 2)
    gate_b = remote(gsend.at[pl.ds(2, 2)], g_b, "B", "gate_ab", 2)
    gate_c = remote(gsend.at[pl.ds(1, 1)], g_c.at[pl.ds(0, 1)], "C", "gate_c", 2)
    gate_d = remote(g_a.at[pl.ds(2, 2)], g_d, "B", "gate_d", 2)
    gate_c3 = remote(g_a.at[pl.ds(1, 1)], g_c.at[pl.ds(1, 1)], "C", "gate_c35", 2)
    gate_c5 = remote(g_b.at[pl.ds(1, 1)], g_c.at[pl.ds(2, 1)], "C", "gate_c35", 2)
    gate_c7 = remote(g_d.at[pl.ds(1, 1)], g_c.at[pl.ds(3, 1)], "C", "gate_c7", 2)

    await_all(lsem.at[1], gsend.at[pl.ds(0, 4)])
    ids_v, gates_v = ids[...], gates[...]
    for p, k in enumerate(GATE_ORDER):
        base = (me ^ k) * local_experts
        for e in range(local_experts):
            row = jnp.sum(jnp.where(ids_v == base + e, gates_v, 0.0), axis=0, keepdims=True)
            gsend[p, pl.ds(2 * e, 1), :] = row[:, :half]
            gsend[p, pl.ds(2 * e + 1, 1), :] = row[:, half:]
    await_all(lsem.at[0], xs.at[0])
    pl.semaphore_wait(barrier, 3)
    start(first[0])
    start((gate_a, gate_b))
    start(first[1])
    start((gate_c, core_own))
    start([pieces[0] for pieces in second[0]])

    def pass_first_0():
        arrive(("first", 0), xs.at[2, lower])
        start(onward[0])
        core[2].start()
        arrive("gate_ab", gsend.at[pl.ds(0, 6)])
        start((gate_c3, gate_c5, gate_d))

    def pass_first_1():
        arrive(("first", 1), xs.at[3, lower])
        start(onward[1])
        core[3].start()
        start([pieces[1] for pieces in second[0]])
        start([pieces[0] for pieces in second[1]])

    def pass_diagonal_0():
        arrive(("onward", 0), xs.at[4, lower])
        core[4].start()
        arrive("gate_d", g_d)
        gate_c7.start()

    def pass_diagonal_1():
        arrive(("onward", 1), xs.at[5, lower])
        core[5].start()

    def pass_second():
        arrive("second", xs.at[pl.ds(6, 2), lower])
        start((core[6], core[7]))

    gate_tiles = {
        0: gsend.at[0], 1: g_c.at[0], 2: g_a.at[0], 3: g_c.at[1],
        4: g_b.at[0], 5: g_c.at[2], 6: g_d.at[0], 7: g_c.at[3],
    }

    def hidden(s, part, e):
        tokens = xs[s, part]
        mask = jnp.concatenate([G[e, part]] * (w1.shape[2] // 128), axis=1) > 0.0
        a = jnp.dot(tokens, w1[e], preferred_element_type=F32)
        b = jnp.dot(tokens, w3[e], preferred_element_type=F32)
        return jnp.where(mask, a * (1.0 / (1.0 + jnp.exp(-a))) * b, 0.0).astype(BF16)

    def experts(s, total, finish, hooks=None, parts=(0, 1)):
        hooks = hooks or {}
        part = pl.ds(parts[0] * half, len(parts) * half)
        left = lax.broadcasted_iota(jnp.int32, (1, half), 1) < QUARTER
        for e in range(local_experts):
            for i in parts:
                (o0, h0, _), (o1, h1, _) = BLOCKS[s][2 * i:2 * i + 2]
                row = gate_tiles[o0][pl.ds(2 * e + h0, 1), :]
                if (o0, h0) != (o1, h1):
                    row = jnp.where(left, row, gate_tiles[o1][pl.ds(2 * e + h1, 1), :])
                G[e, pl.ds(i * half, half), :] = jnp.broadcast_to(row, (half, half)).T
        act = None
        for e in range(local_experts + 1):
            for hook in hooks.get(e, ()):
                hook()
            later = hidden(s, part, e) if e < local_experts else None
            if act is not None:
                out = jnp.dot(act, w2[e - 1], preferred_element_type=F32)
                out = out * jnp.concatenate([G[e - 1, part]] * (w2.shape[2] // 128), axis=1)
                if e == 1:
                    total[part, :] = out
                elif e < local_experts:
                    total[part, :] += out
                else:
                    finish(out)
            act = later

    back_c = {s: remote(out_c.at[s - 2], rec_c.at[s - 2], "C", ("back_c", s), 1) for s in range(2, 8)}
    back_own = [remote(out_c1.at[part], rec_c1.at[part], "C", "back_own", 1) for part in (upper, lower)]

    def finish_own(out):
        own[...] = own[...] + out

    def finish_core_own(part):
        def finish(out):
            out_c1[part, :] = (acc[0, part, :] + out).astype(BF16)
        return finish

    def finish_core(s):
        def finish(out):
            out_c[s - 2] = (acc[s % 2, upper, :] + out[:half]).astype(BF16)
        return finish

    def finish_chip(s):
        def finish(out):
            acc[s % 2, lower, :] += out[-half:]
        return finish

    def send_chip(s):
        i = s - 2
        arrive(("back_c", s), rec_c.at[i])
        if s >= 6:
            arrive(("through", s - 2), d_ab.at[s - 6])
        for j, (owner, h, q) in enumerate(BLOCKS[s][2:]):
            part = pl.ds(j * QUARTER, QUARTER)
            total = acc[s % 2, pl.ds(half + j * QUARTER, QUARTER), :] + rec_c[i, part, :].astype(F32)
            if s >= 6:
                total = total + d_ab[s - 6, 1 if owner == 2 else 0].astype(F32)
            pb[i, part, :] = total.astype(BF16)
            row = pl.ds(token_row(h, q), QUARTER)
            if owner == 6:
                copy = remote(pb.at[i, part], d_ab.at[s - 4, h], "A" if h == 0 else "B", ("through", s), 1)
            else:
                name = ("back", s) if s >= 6 else "back"
                to, dst = ("A", r_a.at[row]) if owner == 2 else ("B", r_b.at[row])
                copy = remote(pb.at[i, part], dst, to, name, 1)
            copy.start()

    def pair(s, *hooks):
        def finish(out):
            finish_core(s)(out)
            finish_chip(s)(out)
        if s < 7:
            arrive(("core", s), xs.at[s, upper] if s < 6 else xs.at[pl.ds(6, 2), upper])
        experts(s, acc.at[s % 2], finish, {2: hooks})
        back_c[s].start()

    do = functools.partial
    experts(0, own, finish_own, {e: [do(await_weights, e)] for e in range(local_experts + 1)})
    pass_first_0()
    arrive("core_own", xs.at[1])
    arrive("gate_c", g_c.at[pl.ds(0, 1)])
    experts(1, acc.at[0], finish_core_own(upper), parts=(0,))
    back_own[0].start()
    arrive("gate_c35", g_c.at[pl.ds(1, 2)])
    pair(2, pass_first_1)
    pair(3, do(send_chip, 2), pass_diagonal_0)
    arrive("gate_c7", g_c.at[pl.ds(3, 1)])
    pair(4, do(send_chip, 3), pass_diagonal_1)
    pair(5, do(send_chip, 4), pass_second)
    pair(6, do(send_chip, 5))
    experts(7, acc.at[1], finish_core(7), {3: [do(send_chip, 6)]}, parts=(0,))
    back_c[7].start()
    experts(7, acc.at[1], finish_chip(7), parts=(1,))
    send_chip(7)
    experts(1, acc.at[0], finish_core_own(lower), parts=(1,))
    back_own[1].start()

    own[...] = own[...] + xs[0].astype(F32)
    arrive("back", r_a)
    own[upper, :] = own[upper, :] + r_a[upper, :].astype(F32)
    own[lower, :] = own[lower, :] + r_b[lower, :].astype(F32)
    arrive("back_own", rec_c1)
    for s in (6, 7):
        arrive(("back", s), r_a.at[upper])
        for owner, h, q in BLOCKS[s][2:]:
            row = pl.ds(token_row(h, q), QUARTER)
            last = (r_a if owner == 2 else r_b)[row, :].astype(F32)
            y_ref[row, :] = (own[row, :] + rec_c1[row, :].astype(F32) + last).astype(BF16)
    await_all(ssem.at[0], xs.at[pl.ds(0, 7)])
    await_all(ssem.at[1], xs.at[pl.ds(0, 7)])
    await_all(ssem.at[2], G.at[0, pl.ds(0, 96)])


def solution(mesh):
    axes = tuple(mesh.axis_names)
    row_spec, w_spec = P(axes, None), P(axes, None, None)

    def local_layer(tokens, expert_ids, gate_weights, w_gate, w_up, w_down):
        rows, width = tokens.shape
        experts, _, ff = w_gate.shape
        top_k = expert_ids.shape[1]
        return pl.pallas_call(
            moe_kernel,
            name="moe_layer",
            out_shape=jax.ShapeDtypeStruct((rows, width), BF16),
            in_specs=[pl.BlockSpec(memory_space=pltpu.HBM)] * 6,
            out_specs=pl.BlockSpec(memory_space=pltpu.VMEM),
            scratch_shapes=[
                pltpu.VMEM((8, rows, width), BF16),
                pltpu.VMEM((experts, width, ff), BF16),
                pltpu.VMEM((experts, width, ff), BF16),
                pltpu.VMEM((experts, ff, width), BF16),
                pltpu.VMEM((top_k, rows), jnp.int32),
                pltpu.VMEM((top_k, rows), F32),
                pltpu.VMEM((8, 8, 128), F32),
                pltpu.VMEM((4, 8, 128), F32),
                pltpu.VMEM((2, 8, 128), F32),
                pltpu.VMEM((2, 8, 128), F32),
                pltpu.VMEM((4, 8, 128), F32),
                pltpu.VMEM((experts, rows, 128), F32),
                pltpu.VMEM((2, rows, width), F32),
                pltpu.VMEM((rows, width), F32),
                pltpu.VMEM((rows, width), BF16),
                pltpu.VMEM((rows, width), BF16),
                pltpu.VMEM((6, rows // 2, width), BF16),
                pltpu.VMEM((6, rows // 2, width), BF16),
                pltpu.VMEM((6, rows // 2, width), BF16),
                pltpu.VMEM((rows, width), BF16),
                pltpu.VMEM((rows, width), BF16),
                pltpu.VMEM((2, 2, QUARTER, width), BF16),
                pltpu.SemaphoreType.DMA((7,)),
                pltpu.SemaphoreType.DMA((3,)),
                pltpu.SemaphoreType.DMA((28,)),
            ],
            compiler_params=pltpu.CompilerParams(
                collective_id=0, has_side_effects=True, vmem_limit_bytes=46 * 2**20
            ),
        )(*(pltpu.with_memory_space_constraint(v, pltpu.HBM) for v in (tokens, expert_ids.T, gate_weights.T, w_gate, w_up, w_down)))

    return jax.shard_map(
        local_layer, mesh=mesh,
        in_specs=(row_spec, row_spec, row_spec, w_spec, w_spec, w_spec),
        out_specs=row_spec, check_vma=False,
    )
```

```python
import functools

import jax
import jax.numpy as jnp
from jax import lax
from jax.experimental import pallas as pl
from jax.experimental.pallas import tpu as pltpu
from jax.sharding import PartitionSpec as P

MESH = pl.DeviceIdType.MESH
F32, BF16 = jnp.float32, jnp.bfloat16

BLOCKS = (
    ((0, 0, 0), (0, 0, 1), (0, 1, 0), (0, 1, 1)),
    ((1, 0, 0), (1, 0, 1), (1, 1, 0), (1, 1, 1)),
    ((3, 0, 0), (5, 1, 1), (2, 0, 0), (4, 1, 1)),
    ((5, 1, 0), (3, 0, 1), (4, 1, 0), (2, 0, 1)),
    ((7, 0, 0), (7, 1, 1), (6, 0, 0), (6, 1, 1)),
    ((7, 1, 0), (7, 0, 1), (6, 1, 0), (6, 0, 1)),
    ((5, 0, 0), (3, 1, 1), (4, 0, 0), (2, 1, 1)),
    ((3, 1, 0), (5, 0, 1), (2, 1, 0), (4, 0, 1)),
)
GATE_ORDER = (0, 1, 4, 5, 2, 3, 6, 7)
QUARTER = 64


def place(piece):
    for s, pieces in enumerate(BLOCKS):
        if piece in pieces:
            return s, pieces.index(piece) * QUARTER


def token_row(half, quarter):
    return (2 * half + quarter) * QUARTER


def moe_kernel(
    x_hbm, ids_hbm, gates_hbm, w1_hbm, w3_hbm, w2_hbm, y_ref,
    xs, w1, w3, w2, ids, gates, gsend, g_a, g_b, g_d, g_c, G,
    acc, own, out_c1, rec_c1, out_c, rec_c, pb, r_a, r_b, d_ab, lsem, ssem, rsem,
):
    z, y, x = lax.axis_index("ez"), lax.axis_index("ey"), lax.axis_index("ex")
    me = 4 * z + 2 * y + x
    dev = {"A": (z, 1 - y, x), "B": (1 - z, y, x), "C": (z, y, 1 - x)}
    half = 2 * QUARTER
    local_experts = w1.shape[0]
    names = {}

    def await_all(sem, like):
        pltpu.make_async_copy(like, like, sem).wait()

    def received(name):
        return rsem.at[names.setdefault(name, len(names))]

    def remote(src, dst, to, name, kind=0):
        return pltpu.make_async_remote_copy(
            src_ref=src, dst_ref=dst, send_sem=ssem.at[kind], recv_sem=received(name),
            device_id=dev[to], device_id_type=MESH,
        )

    def rows(piece, skip=0, size=QUARTER):
        s, row = place(piece)
        return xs.at[s, pl.ds(row + skip, size)]

    def start(copies):
        for copy in copies:
            copy.start()

    def arrive(name, like):
        await_all(received(name), like)

    def load(src, dst, sem):
        pltpu.make_async_copy(src, dst, lsem.at[sem]).start()

    load(ids_hbm, ids, 1)
    load(gates_hbm, gates, 1)
    load(x_hbm, xs.at[0], 0)
    for e in range(local_experts):
        load(w1_hbm.at[e], w1.at[e], 2 + e)
        load(w3_hbm.at[e], w3.at[e], 2 + e)
        load(w2_hbm.at[e], w2.at[e], 3 + e)

    def await_weights(e):
        matrices = 2 * (e < local_experts) + (e > 0)
        await_all(lsem.at[2 + e], w1.at[pl.ds(0, matrices)])

    barrier = pltpu.get_barrier_semaphore()
    for to in "ABC":
        pl.semaphore_signal(barrier, inc=1, device_id=dev[to], device_id_type=MESH)

    first, second, onward = ([], []), ([], []), ([], [])
    for i in range(2):
        s1, s3 = 2 + i, 6 + i
        for owner, h, q in BLOCKS[s1][2:]:
            to, across = ("A", "B") if owner == 2 else ("B", "A")
            first[i].append(remote(rows((0, h, q)), rows((owner, h, q)), to, ("first", i)))
            onward[i].append(remote(rows((owner, h, q)), rows((6, h, q)), across, ("onward", i)))
        for owner, h, q in BLOCKS[s3][2:]:
            to = "A" if owner == 2 else "B"
            cuts = ((0, 32), (32, 32)) if i == 0 else ((0, QUARTER),)
            second[i].append([remote(rows((0, h, q), *cut), rows((owner, h, q), *cut), to, "second") for cut in cuts])
    core_own = remote(xs.at[0], xs.at[1], "C", "core_own")
    upper, lower = pl.ds(0, half), pl.ds(half, half)
    core = {s: remote(xs.at[s, lower], xs.at[s, upper], "C", ("core", min(s, 6))) for s in range(2, 8)}
    gate_a = remote(gsend.at[pl.ds(4, 4)], g_a, "A", "gate_ab", 2)
    gate_b = remote(gsend.at[pl.ds(2, 2)], g_b, "B", "gate_ab", 2)
    gate_c = remote(gsend.at[pl.ds(1, 1)], g_c.at[pl.ds(0, 1)], "C", "gate_c", 2)
    gate_d = remote(g_a.at[pl.ds(2, 2)], g_d, "B", "gate_d", 2)
    gate_c3 = remote(g_a.at[pl.ds(1, 1)], g_c.at[pl.ds(1, 1)], "C", "gate_c35", 2)
    gate_c5 = remote(g_b.at[pl.ds(1, 1)], g_c.at[pl.ds(2, 1)], "C", "gate_c35", 2)
    gate_c7 = remote(g_d.at[pl.ds(1, 1)], g_c.at[pl.ds(3, 1)], "C", "gate_c7", 2)

    await_all(lsem.at[1], gsend.at[pl.ds(0, 4)])
    ids_v, gates_v = ids[...], gates[...]
    for p, k in enumerate(GATE_ORDER):
        base = (me ^ k) * local_experts
        for e in range(local_experts):
            row = jnp.sum(jnp.where(ids_v == base + e, gates_v, 0.0), axis=0, keepdims=True)
            gsend[p, pl.ds(2 * e, 1), :] = row[:, :half]
            gsend[p, pl.ds(2 * e + 1, 1), :] = row[:, half:]
    await_all(lsem.at[0], xs.at[0])
    pl.semaphore_wait(barrier, 3)
    start(first[0])
    start((gate_a, gate_b))
    start(first[1])
    start((gate_c, core_own))
    start([pieces[0] for pieces in second[0]])

    def pass_first_0():
        arrive(("first", 0), xs.at[2, lower])
        start(onward[0])
        core[2].start()
        arrive("gate_ab", gsend.at[pl.ds(0, 6)])
        start((gate_c3, gate_c5, gate_d))

    def pass_first_1():
        arrive(("first", 1), xs.at[3, lower])
        start(onward[1])
        core[3].start()
        start([pieces[1] for pieces in second[0]])
        start([pieces[0] for pieces in second[1]])

    def pass_diagonal_0():
        arrive(("onward", 0), xs.at[4, lower])
        core[4].start()
        arrive("gate_d", g_d)
        gate_c7.start()

    def pass_diagonal_1():
        arrive(("onward", 1), xs.at[5, lower])
        core[5].start()

    def pass_second():
        arrive("second", xs.at[pl.ds(6, 2), lower])
        start((core[6], core[7]))

    gate_tiles = {
        0: gsend.at[0], 1: g_c.at[0], 2: g_a.at[0], 3: g_c.at[1],
        4: g_b.at[0], 5: g_c.at[2], 6: g_d.at[0], 7: g_c.at[3],
    }

    def hidden(s, part, e):
        tokens = xs[s, part]
        mask = jnp.concatenate([G[e, part]] * (w1.shape[2] // 128), axis=1) > 0.0
        a = jnp.dot(tokens, w1[e], preferred_element_type=F32)
        b = jnp.dot(tokens, w3[e], preferred_element_type=F32)
        return jnp.where(mask, a * (1.0 / (1.0 + jnp.exp(-a))) * b, 0.0).astype(BF16)

    def experts(s, total, finish, hooks=None, parts=(0, 1)):
        hooks = hooks or {}
        part = pl.ds(parts[0] * half, len(parts) * half)
        left = lax.broadcasted_iota(jnp.int32, (1, half), 1) < QUARTER
        for e in range(local_experts):
            for i in parts:
                (o0, h0, _), (o1, h1, _) = BLOCKS[s][2 * i:2 * i + 2]
                row = gate_tiles[o0][pl.ds(2 * e + h0, 1), :]
                if (o0, h0) != (o1, h1):
                    row = jnp.where(left, row, gate_tiles[o1][pl.ds(2 * e + h1, 1), :])
                G[e, pl.ds(i * half, half), :] = jnp.broadcast_to(row, (half, half)).T
        act = None
        for e in range(local_experts + 1):
            for hook in hooks.get(e, ()):
                hook()
            later = hidden(s, part, e) if e < local_experts else None
            if act is not None:
                out = jnp.dot(act, w2[e - 1], preferred_element_type=F32)
                out = out * jnp.concatenate([G[e - 1, part]] * (w2.shape[2] // 128), axis=1)
                if e == 1:
                    total[part, :] = out
                elif e < local_experts:
                    total[part, :] += out
                else:
                    finish(out)
            act = later

    back_c = {s: remote(out_c.at[s - 2], rec_c.at[s - 2], "C", ("back_c", s), 1) for s in range(2, 8)}
    back_own = [remote(out_c1.at[part], rec_c1.at[part], "C", "back_own", 1) for part in (upper, lower)]

    def finish_own(out):
        own[...] = own[...] + out

    def finish_core_own(part):
        def finish(out):
            out_c1[part, :] = (acc[0, part, :] + out).astype(BF16)
        return finish

    def finish_core(s):
        def finish(out):
            out_c[s - 2] = (acc[s % 2, upper, :] + out[:half]).astype(BF16)
        return finish

    def finish_chip(s):
        def finish(out):
            acc[s % 2, lower, :] += out[-half:]
        return finish

    held = []

    def send_chip(s):
        i = s - 2
        arrive(("back_c", s), rec_c.at[i])
        if s >= 6:
            arrive(("through", s - 2), d_ab.at[s - 6])
        for j, (owner, h, q) in enumerate(BLOCKS[s][2:]):
            part = pl.ds(j * QUARTER, QUARTER)
            total = acc[s % 2, pl.ds(half + j * QUARTER, QUARTER), :] + rec_c[i, part, :].astype(F32)
            if s >= 6:
                total = total + d_ab[s - 6, 1 if owner == 2 else 0].astype(F32)
            pb[i, part, :] = total.astype(BF16)
            row = pl.ds(token_row(h, q), QUARTER)
            if owner == 6:
                copy = remote(pb.at[i, part], d_ab.at[s - 4, h], "A" if h == 0 else "B", ("through", s), 1)
            elif s == 3:
                to, dst = ("A", r_a) if owner == 2 else ("B", r_b)
                rest, copy = (
                    remote(pb.at[i, pl.ds(j * QUARTER + skip, 32)], dst.at[pl.ds(token_row(h, q) + skip, 32)], to, "back", 1)
                    for skip in (32, 0)
                )
                held.append(rest)
            else:
                name = ("back", s) if s >= 6 else "back"
                to, dst = ("A", r_a.at[row]) if owner == 2 else ("B", r_b.at[row])
                copy = remote(pb.at[i, part], dst, to, name, 1)
            copy.start()
        if s == 4:
            start(held)

    def pair(s, *hooks):
        def finish(out):
            finish_core(s)(out)
            finish_chip(s)(out)
        if s < 7:
            arrive(("core", s), xs.at[s, upper] if s < 6 else xs.at[pl.ds(6, 2), upper])
        experts(s, acc.at[s % 2], finish, {2: hooks})
        back_c[s].start()

    do = functools.partial
    experts(0, own, finish_own, {e: [do(await_weights, e)] for e in range(local_experts + 1)})
    pass_first_0()
    arrive("core_own", xs.at[1])
    arrive("gate_c", g_c.at[pl.ds(0, 1)])
    experts(1, acc.at[0], finish_core_own(upper), parts=(0,))
    back_own[0].start()
    arrive("gate_c35", g_c.at[pl.ds(1, 2)])
    pair(2, pass_first_1)
    pair(3, do(send_chip, 2), pass_diagonal_0)
    arrive("gate_c7", g_c.at[pl.ds(3, 1)])
    pair(4, do(send_chip, 3), pass_diagonal_1)
    pair(5, do(send_chip, 4), pass_second)
    pair(6, do(send_chip, 5))
    experts(7, acc.at[1], finish_core(7), {3: [do(send_chip, 6)]}, parts=(0,))
    back_c[7].start()
    experts(7, acc.at[1], finish_chip(7), parts=(1,))
    pl.when(x == 0)(do(send_chip, 7))
    experts(1, acc.at[0], finish_core_own(lower), {3: [do(pl.when(x == 1), do(send_chip, 7))]}, parts=(1,))
    back_own[1].start()

    own[...] = own[...] + xs[0].astype(F32)
    arrive("back", r_a)
    own[upper, :] = own[upper, :] + r_a[upper, :].astype(F32)
    own[lower, :] = own[lower, :] + r_b[lower, :].astype(F32)
    arrive("back_own", rec_c1)
    for s in (6, 7):
        arrive(("back", s), r_a.at[upper])
        for owner, h, q in BLOCKS[s][2:]:
            row = pl.ds(token_row(h, q), QUARTER)
            last = (r_a if owner == 2 else r_b)[row, :].astype(F32)
            y_ref[row, :] = (own[row, :] + rec_c1[row, :].astype(F32) + last).astype(BF16)
    await_all(ssem.at[0], xs.at[pl.ds(0, 7)])
    await_all(ssem.at[1], xs.at[pl.ds(0, 7)])
    await_all(ssem.at[2], G.at[0, pl.ds(0, 96)])


def solution(mesh):
    axes = tuple(mesh.axis_names)
    row_spec, w_spec = P(axes, None), P(axes, None, None)

    def local_layer(tokens, expert_ids, gate_weights, w_gate, w_up, w_down):
        rows, width = tokens.shape
        experts, _, ff = w_gate.shape
        top_k = expert_ids.shape[1]
        return pl.pallas_call(
            moe_kernel,
            name="moe_layer",
            out_shape=jax.ShapeDtypeStruct((rows, width), BF16),
            in_specs=[pl.BlockSpec(memory_space=pltpu.HBM)] * 6,
            out_specs=pl.BlockSpec(memory_space=pltpu.VMEM),
            scratch_shapes=[
                pltpu.VMEM((8, rows, width), BF16),
                pltpu.VMEM((experts, width, ff), BF16),
                pltpu.VMEM((experts, width, ff), BF16),
                pltpu.VMEM((experts, ff, width), BF16),
                pltpu.VMEM((top_k, rows), jnp.int32),
                pltpu.VMEM((top_k, rows), F32),
                pltpu.VMEM((8, 8, 128), F32),
                pltpu.VMEM((4, 8, 128), F32),
                pltpu.VMEM((2, 8, 128), F32),
                pltpu.VMEM((2, 8, 128), F32),
                pltpu.VMEM((4, 8, 128), F32),
                pltpu.VMEM((experts, rows, 128), F32),
                pltpu.VMEM((2, rows, width), F32),
                pltpu.VMEM((rows, width), F32),
                pltpu.VMEM((rows, width), BF16),
                pltpu.VMEM((rows, width), BF16),
                pltpu.VMEM((6, rows // 2, width), BF16),
                pltpu.VMEM((6, rows // 2, width), BF16),
                pltpu.VMEM((6, rows // 2, width), BF16),
                pltpu.VMEM((rows, width), BF16),
                pltpu.VMEM((rows, width), BF16),
                pltpu.VMEM((2, 2, QUARTER, width), BF16),
                pltpu.SemaphoreType.DMA((7,)),
                pltpu.SemaphoreType.DMA((3,)),
                pltpu.SemaphoreType.DMA((28,)),
            ],
            compiler_params=pltpu.CompilerParams(
                collective_id=0, has_side_effects=True, vmem_limit_bytes=46 * 2**20
            ),
        )(*(pltpu.with_memory_space_constraint(v, pltpu.HBM) for v in (tokens, expert_ids.T, gate_weights.T, w_gate, w_up, w_down)))

    return jax.shard_map(
        local_layer, mesh=mesh,
        in_specs=(row_spec, row_spec, row_spec, w_spec, w_spec, w_spec),
        out_specs=row_spec, check_vma=False,
    )
```

```python
import functools

import jax
import jax.numpy as jnp
from jax import lax
from jax.experimental import pallas as pl
from jax.experimental.pallas import tpu as pltpu
from jax.sharding import PartitionSpec as P

MESH = pl.DeviceIdType.MESH
F32, BF16 = jnp.float32, jnp.bfloat16

BLOCKS = (
    ((0, 0, 0), (0, 0, 1), (0, 1, 0), (0, 1, 1)),
    ((1, 0, 0), (1, 0, 1), (1, 1, 0), (1, 1, 1)),
    ((3, 0, 0), (5, 1, 1), (2, 0, 0), (4, 1, 1)),
    ((5, 1, 0), (3, 0, 1), (4, 1, 0), (2, 0, 1)),
    ((7, 0, 0), (7, 1, 1), (6, 0, 0), (6, 1, 1)),
    ((7, 1, 0), (7, 0, 1), (6, 1, 0), (6, 0, 1)),
    ((5, 0, 0), (3, 1, 1), (4, 0, 0), (2, 1, 1)),
    ((3, 1, 0), (5, 0, 1), (2, 1, 0), (4, 0, 1)),
)
GATE_ORDER = (0, 1, 4, 5, 2, 3, 6, 7)
QUARTER = 64


def place(piece):
    for s, pieces in enumerate(BLOCKS):
        if piece in pieces:
            return s, pieces.index(piece) * QUARTER


def token_row(half, quarter):
    return (2 * half + quarter) * QUARTER


def moe_kernel(
    x_hbm, ids_hbm, gates_hbm, w1_hbm, w3_hbm, w2_hbm, y_ref,
    xs, w1, w3, w2, ids, gates, gsend, g_a, g_b, g_d, g_c, G,
    acc, own, out_c1, rec_c1, out_c, rec_c, pb, r_a, r_b, d_ab, lsem, ssem, rsem,
):
    z, y, x = lax.axis_index("ez"), lax.axis_index("ey"), lax.axis_index("ex")
    me = 4 * z + 2 * y + x
    dev = {"A": (z, 1 - y, x), "B": (1 - z, y, x), "C": (z, y, 1 - x)}
    half = 2 * QUARTER
    local_experts = w1.shape[0]
    names = {}

    def await_all(sem, like):
        pltpu.make_async_copy(like, like, sem).wait()

    def received(name):
        return rsem.at[names.setdefault(name, len(names))]

    def remote(src, dst, to, name, kind=0):
        return pltpu.make_async_remote_copy(
            src_ref=src, dst_ref=dst, send_sem=ssem.at[kind], recv_sem=received(name),
            device_id=dev[to], device_id_type=MESH,
        )

    def rows(piece, skip=0, size=QUARTER):
        s, row = place(piece)
        return xs.at[s, pl.ds(row + skip, size)]

    def start(copies):
        for copy in copies:
            copy.start()

    def arrive(name, like):
        await_all(received(name), like)

    def load(src, dst, sem):
        pltpu.make_async_copy(src, dst, lsem.at[sem]).start()

    load(x_hbm, xs.at[0], 0)
    load(ids_hbm, ids, 1)
    load(gates_hbm, gates, 1)
    for e in range(local_experts):
        load(w1_hbm.at[e], w1.at[e], 2 + e)
        load(w3_hbm.at[e], w3.at[e], 2 + e)
        load(w2_hbm.at[e], w2.at[e], 3 + e)

    def await_weights(e):
        matrices = 2 * (e < local_experts) + (e > 0)
        await_all(lsem.at[2 + e], w1.at[pl.ds(0, matrices)])

    barrier = pltpu.get_barrier_semaphore()
    for to in "ABC":
        pl.semaphore_signal(barrier, inc=1, device_id=dev[to], device_id_type=MESH)

    first, second, onward = ([], []), ([], []), ([], [])
    for i in range(2):
        s1, s3 = 2 + i, 6 + i
        for owner, h, q in BLOCKS[s1][2:]:
            to, across = ("A", "B") if owner == 2 else ("B", "A")
            first[i].append(remote(rows((0, h, q)), rows((owner, h, q)), to, ("first", i)))
            onward[i].append(remote(rows((owner, h, q)), rows((6, h, q)), across, ("onward", i)))
        for owner, h, q in BLOCKS[s3][2:]:
            to = "A" if owner == 2 else "B"
            cuts = ((0, 32), (32, 32)) if i == 0 else ((0, QUARTER),)
            second[i].append([remote(rows((0, h, q), *cut), rows((owner, h, q), *cut), to, "second") for cut in cuts])
    core_own = remote(xs.at[0], xs.at[1], "C", "core_own")
    upper, lower = pl.ds(0, half), pl.ds(half, half)
    core = {s: remote(xs.at[s, lower], xs.at[s, upper], "C", ("core", min(s, 6))) for s in range(2, 8)}
    gate_a = remote(gsend.at[pl.ds(4, 4)], g_a, "A", "gate_ab", 2)
    gate_b = remote(gsend.at[pl.ds(2, 2)], g_b, "B", "gate_ab", 2)
    gate_c = remote(gsend.at[pl.ds(1, 1)], g_c.at[pl.ds(0, 1)], "C", "gate_c", 2)
    gate_d = remote(g_a.at[pl.ds(2, 2)], g_d, "B", "gate_d", 2)
    gate_c3 = remote(g_a.at[pl.ds(1, 1)], g_c.at[pl.ds(1, 1)], "C", "gate_c35", 2)
    gate_c5 = remote(g_b.at[pl.ds(1, 1)], g_c.at[pl.ds(2, 1)], "C", "gate_c35", 2)
    gate_c7 = remote(g_d.at[pl.ds(1, 1)], g_c.at[pl.ds(3, 1)], "C", "gate_c7", 2)

    await_all(lsem.at[1], gsend.at[pl.ds(0, 4)])
    ids_v, gates_v = ids[...], gates[...]
    for p, k in enumerate(GATE_ORDER):
        base = (me ^ k) * local_experts
        for e in range(local_experts):
            row = jnp.sum(jnp.where(ids_v == base + e, gates_v, 0.0), axis=0, keepdims=True)
            gsend[p, pl.ds(2 * e, 1), :] = row[:, :half]
            gsend[p, pl.ds(2 * e + 1, 1), :] = row[:, half:]
    await_all(lsem.at[0], xs.at[0])
    pl.semaphore_wait(barrier, 3)
    start(first[0])
    start((gate_a, gate_b))
    start(first[1])
    start((gate_c, core_own))
    start([pieces[0] for pieces in second[0]])

    def pass_first_0():
        arrive(("first", 0), xs.at[2, lower])
        start(onward[0])
        core[2].start()
        arrive("gate_ab", gsend.at[pl.ds(0, 6)])
        start((gate_c3, gate_c5, gate_d))

    def pass_first_1():
        arrive(("first", 1), xs.at[3, lower])
        start(onward[1])
        core[3].start()
        start([pieces[1] for pieces in second[0]])
        start([pieces[0] for pieces in second[1]])

    def pass_diagonal_0():
        arrive(("onward", 0), xs.at[4, lower])
        core[4].start()
        arrive("gate_d", g_d)
        gate_c7.start()

    def pass_diagonal_1():
        arrive(("onward", 1), xs.at[5, lower])
        core[5].start()

    def pass_second():
        arrive("second", xs.at[pl.ds(6, 2), lower])
        start((core[6], core[7]))

    gate_tiles = {
        0: gsend.at[0], 1: g_c.at[0], 2: g_a.at[0], 3: g_c.at[1],
        4: g_b.at[0], 5: g_c.at[2], 6: g_d.at[0], 7: g_c.at[3],
    }

    def hidden(s, part, e):
        tokens = xs[s, part]
        mask = jnp.concatenate([G[e, part]] * (w1.shape[2] // 128), axis=1) > 0.0
        a = jnp.dot(tokens, w1[e], preferred_element_type=F32)
        b = jnp.dot(tokens, w3[e], preferred_element_type=F32)
        return jnp.where(mask, a * (1.0 / (1.0 + jnp.exp(-a))) * b, 0.0).astype(BF16)

    def experts(s, total, finish, hooks=None, parts=(0, 1), part=None):
        hooks = hooks or {}
        part = part or pl.ds(parts[0] * half, len(parts) * half)
        left = lax.broadcasted_iota(jnp.int32, (1, half), 1) < QUARTER
        for e in range(local_experts):
            for i in parts:
                (o0, h0, _), (o1, h1, _) = BLOCKS[s][2 * i:2 * i + 2]
                row = gate_tiles[o0][pl.ds(2 * e + h0, 1), :]
                if (o0, h0) != (o1, h1):
                    row = jnp.where(left, row, gate_tiles[o1][pl.ds(2 * e + h1, 1), :])
                G[e, pl.ds(i * half, half), :] = jnp.broadcast_to(row, (half, half)).T
        act = None
        for e in range(local_experts + 1):
            for hook in hooks.get(e, ()):
                hook()
            later = hidden(s, part, e) if e < local_experts else None
            if act is not None:
                out = jnp.dot(act, w2[e - 1], preferred_element_type=F32)
                out = out * jnp.concatenate([G[e - 1, part]] * (w2.shape[2] // 128), axis=1)
                if e == 1:
                    total[part, :] = out
                elif e < local_experts:
                    total[part, :] += out
                else:
                    finish(out)
            act = later

    back_c = {s: remote(out_c.at[s - 2], rec_c.at[s - 2], "C", ("back_c", s), 1) for s in range(2, 8)}
    back_own = [remote(out_c1.at[part], rec_c1.at[part], "C", "back_own", 1) for part in (upper, lower)]

    def finish_own(out):
        own[...] = own[...] + out

    def finish_core_own(part):
        def finish(out):
            out_c1[part, :] = (acc[0, part, :] + out).astype(BF16)
        return finish

    held = []

    def send_chip(s):
        i = s - 2
        arrive(("back_c", s), rec_c.at[i])
        if s >= 6:
            arrive(("through", s - 2), d_ab.at[s - 6])
        for j, (owner, h, q) in enumerate(BLOCKS[s][2:]):
            part = pl.ds(j * QUARTER, QUARTER)
            total = acc[s % 2, pl.ds(half + j * QUARTER, QUARTER), :] + rec_c[i, part, :].astype(F32)
            if s >= 6:
                total = total + d_ab[s - 6, 1 if owner == 2 else 0].astype(F32)
            pb[i, part, :] = total.astype(BF16)
            row = pl.ds(token_row(h, q), QUARTER)
            if owner == 6:
                copy = remote(pb.at[i, part], d_ab.at[s - 4, h], "A" if h == 0 else "B", ("through", s), 1)
            elif s == 3:
                to, dst = ("A", r_a) if owner == 2 else ("B", r_b)
                rest, copy = (
                    remote(pb.at[i, pl.ds(j * QUARTER + skip, 32)], dst.at[pl.ds(token_row(h, q) + skip, 32)], to, "back", 1)
                    for skip in (32, 0)
                )
                held.append(rest)
            else:
                name = ("back", s) if s >= 6 else "back"
                to, dst = ("A", r_a.at[row]) if owner == 2 else ("B", r_b.at[row])
                copy = remote(pb.at[i, part], dst, to, name, 1)
            copy.start()
        if s == 4:
            start(held)

    def pair(s, *hooks):
        def finish(out):
            out_c[s - 2] = (acc[s % 2, upper, :] + out[:half]).astype(BF16)
            acc[s % 2, lower, :] += out[half:]
        arrive(("core", s), xs.at[s, upper] if s < 6 else xs.at[pl.ds(6, 2), upper])
        experts(s, acc.at[s % 2], finish, {2: hooks})
        back_c[s].start()

    do = functools.partial
    experts(0, own, finish_own, {e: [do(await_weights, e)] for e in range(local_experts + 1)})
    pass_first_0()
    arrive("core_own", xs.at[1])
    arrive("gate_c", g_c.at[pl.ds(0, 1)])
    experts(1, acc.at[0], finish_core_own(upper), parts=(0,))
    back_own[0].start()
    arrive("gate_c35", g_c.at[pl.ds(1, 2)])
    pair(2, pass_first_1)
    pair(3, do(send_chip, 2), pass_diagonal_0)
    arrive("gate_c7", g_c.at[pl.ds(3, 1)])
    pair(4, do(send_chip, 3), pass_diagonal_1)
    pair(5, do(send_chip, 4), pass_second)
    pair(6, do(send_chip, 5))
    near, far = (pl.ds(pl.multiple_of(i * half, half), half) for i in (1 - x, x))

    def finish_half(part):
        def finish(out):
            acc[1, part, :] += out
        return finish

    def exchange():
        out_c[5] = acc[1, upper, :].astype(BF16)
        back_c[7].start()

    experts(7, acc.at[1], finish_half(near), {3: [do(send_chip, 6)]}, part=near)
    pl.when(x == 1)(exchange)
    experts(7, acc.at[1], finish_half(far), {3: [do(pl.when(x == 0), do(send_chip, 7))]}, parts=(), part=far)
    pl.when(x == 0)(exchange)
    experts(1, acc.at[0], finish_core_own(lower), {2: [do(pl.when(x == 1), do(send_chip, 7))]}, parts=(1,))
    back_own[1].start()

    own[...] = own[...] + xs[0].astype(F32)
    arrive("back", r_a)
    own[upper, :] = own[upper, :] + r_a[upper, :].astype(F32)
    own[lower, :] = own[lower, :] + r_b[lower, :].astype(F32)
    arrive("back_own", rec_c1)
    for s in (6, 7):
        arrive(("back", s), r_a.at[upper])
        for owner, h, q in BLOCKS[s][2:]:
            row = pl.ds(token_row(h, q), QUARTER)
            last = (r_a if owner == 2 else r_b)[row, :].astype(F32)
            y_ref[row, :] = (own[row, :] + rec_c1[row, :].astype(F32) + last).astype(BF16)
    await_all(ssem.at[0], xs.at[pl.ds(0, 7)])
    await_all(ssem.at[1], xs.at[pl.ds(0, 7)])
    await_all(ssem.at[2], G.at[0, pl.ds(0, 96)])


def solution(mesh):
    axes = tuple(mesh.axis_names)
    row_spec, w_spec = P(axes, None), P(axes, None, None)

    def local_layer(tokens, expert_ids, gate_weights, w_gate, w_up, w_down):
        rows, width = tokens.shape
        experts, _, ff = w_gate.shape
        top_k = expert_ids.shape[1]
        return pl.pallas_call(
            moe_kernel,
            name="moe_layer",
            out_shape=jax.ShapeDtypeStruct((rows, width), BF16),
            in_specs=[pl.BlockSpec(memory_space=pltpu.HBM)] * 6,
            out_specs=pl.BlockSpec(memory_space=pltpu.VMEM),
            scratch_shapes=[
                pltpu.VMEM((8, rows, width), BF16),
                pltpu.VMEM((experts, width, ff), BF16),
                pltpu.VMEM((experts, width, ff), BF16),
                pltpu.VMEM((experts, ff, width), BF16),
                pltpu.VMEM((top_k, rows), jnp.int32),
                pltpu.VMEM((top_k, rows), F32),
                pltpu.VMEM((8, 8, 128), F32),
                pltpu.VMEM((4, 8, 128), F32),
                pltpu.VMEM((2, 8, 128), F32),
                pltpu.VMEM((2, 8, 128), F32),
                pltpu.VMEM((4, 8, 128), F32),
                pltpu.VMEM((experts, rows, 128), F32),
                pltpu.VMEM((2, rows, width), F32),
                pltpu.VMEM((rows, width), F32),
                pltpu.VMEM((rows, width), BF16),
                pltpu.VMEM((rows, width), BF16),
                pltpu.VMEM((6, rows // 2, width), BF16),
                pltpu.VMEM((6, rows // 2, width), BF16),
                pltpu.VMEM((6, rows // 2, width), BF16),
                pltpu.VMEM((rows, width), BF16),
                pltpu.VMEM((rows, width), BF16),
                pltpu.VMEM((2, 2, QUARTER, width), BF16),
                pltpu.SemaphoreType.DMA((7,)),
                pltpu.SemaphoreType.DMA((3,)),
                pltpu.SemaphoreType.DMA((28,)),
            ],
            compiler_params=pltpu.CompilerParams(
                collective_id=0, has_side_effects=True, vmem_limit_bytes=46 * 2**20
            ),
        )(*(pltpu.with_memory_space_constraint(v, pltpu.HBM) for v in (tokens, expert_ids.T, gate_weights.T, w_gate, w_up, w_down)))

    return jax.shard_map(
        local_layer, mesh=mesh,
        in_specs=(row_spec, row_spec, row_spec, w_spec, w_spec, w_spec),
        out_specs=row_spec, check_vma=False,
    )
```

```python
import functools

import jax
import jax.numpy as jnp
from jax import lax
from jax.experimental import pallas as pl
from jax.experimental.pallas import tpu as pltpu
from jax.sharding import PartitionSpec as P

MESH = pl.DeviceIdType.MESH
F32, BF16 = jnp.float32, jnp.bfloat16

BLOCKS = (
    ((0, 0, 0), (0, 0, 1), (0, 1, 0), (0, 1, 1)),
    ((1, 0, 0), (1, 0, 1), (1, 1, 0), (1, 1, 1)),
    ((3, 0, 0), (5, 1, 1), (2, 0, 0), (4, 1, 1)),
    ((5, 1, 0), (3, 0, 1), (4, 1, 0), (2, 0, 1)),
    ((7, 0, 0), (7, 1, 1), (6, 0, 0), (6, 1, 1)),
    ((7, 1, 0), (7, 0, 1), (6, 1, 0), (6, 0, 1)),
    ((5, 0, 0), (3, 1, 1), (4, 0, 0), (2, 1, 1)),
    ((3, 1, 0), (5, 0, 1), (2, 1, 0), (4, 0, 1)),
)
GATE_ORDER = (0, 1, 4, 5, 2, 3, 6, 7)
QUARTER = 64


def place(piece):
    for s, pieces in enumerate(BLOCKS):
        if piece in pieces:
            return s, pieces.index(piece) * QUARTER


def token_row(half, quarter):
    return (2 * half + quarter) * QUARTER


def moe_kernel(
    x_hbm, ids_hbm, gates_hbm, w1_hbm, w3_hbm, w2_hbm, y_ref,
    xs, w1, w3, w2, ids, gates, gsend, g_a, g_b, g_d, g_c, G,
    acc, own, out_c1, rec_c1, out_c, rec_c, pb, r_a, r_b, d_ab, lsem, ssem, rsem,
):
    z, y, x = lax.axis_index("ez"), lax.axis_index("ey"), lax.axis_index("ex")
    me = 4 * z + 2 * y + x
    dev = {"A": (z, 1 - y, x), "B": (1 - z, y, x), "C": (z, y, 1 - x)}
    half = 2 * QUARTER
    local_experts = w1.shape[0]
    names = {}

    def await_all(sem, like):
        pltpu.make_async_copy(like, like, sem).wait()

    def received(name):
        return rsem.at[names.setdefault(name, len(names))]

    def remote(src, dst, to, name, kind=0):
        return pltpu.make_async_remote_copy(
            src_ref=src, dst_ref=dst, send_sem=ssem.at[kind], recv_sem=received(name),
            device_id=dev[to], device_id_type=MESH,
        )

    def rows(piece, skip=0, size=QUARTER):
        s, row = place(piece)
        return xs.at[s, pl.ds(row + skip, size)]

    def start(copies):
        for copy in copies:
            copy.start()

    def arrive(name, like):
        await_all(received(name), like)

    def load(src, dst, sem):
        pltpu.make_async_copy(src, dst, lsem.at[sem]).start()

    load(x_hbm, xs.at[0], 0)
    load(ids_hbm, ids, 1)
    load(gates_hbm, gates, 1)
    for e in range(local_experts):
        load(w1_hbm.at[e], w1.at[e], 2 + e)
        load(w3_hbm.at[e], w3.at[e], 2 + e)
        load(w2_hbm.at[e], w2.at[e], 2 + min(e + 1, local_experts - 1))

    def await_weights(e):
        matrices = 2 + (e > 0) + (e == local_experts - 1)
        await_all(lsem.at[2 + e], w1.at[pl.ds(0, matrices)])

    barrier = pltpu.get_barrier_semaphore()
    for to in "ABC":
        pl.semaphore_signal(barrier, inc=1, device_id=dev[to], device_id_type=MESH)

    first, second, onward = ([], []), ([], []), ([], [])
    for i in range(2):
        s1, s3 = 2 + i, 6 + i
        for owner, h, q in BLOCKS[s1][2:]:
            to, across = ("A", "B") if owner == 2 else ("B", "A")
            first[i].append(remote(rows((0, h, q)), rows((owner, h, q)), to, ("first", i)))
            onward[i].append(remote(rows((owner, h, q)), rows((6, h, q)), across, ("onward", i)))
        for owner, h, q in BLOCKS[s3][2:]:
            to = "A" if owner == 2 else "B"
            cuts = ((0, 32), (32, 32)) if i == 0 else ((0, QUARTER),)
            second[i].append([remote(rows((0, h, q), *cut), rows((owner, h, q), *cut), to, "second") for cut in cuts])
    core_own = remote(xs.at[0], xs.at[1], "C", "core_own")
    upper, lower = pl.ds(0, half), pl.ds(half, half)
    core = {s: remote(xs.at[s, lower], xs.at[s, upper], "C", ("core", min(s, 6))) for s in range(2, 8)}
    gate_a = remote(gsend.at[pl.ds(4, 4)], g_a, "A", "gate_ab", 2)
    gate_b = remote(gsend.at[pl.ds(2, 2)], g_b, "B", "gate_ab", 2)
    gate_c = remote(gsend.at[pl.ds(1, 1)], g_c.at[pl.ds(0, 1)], "C", "gate_c", 2)
    gate_d = remote(g_a.at[pl.ds(2, 2)], g_d, "B", "gate_d", 2)
    gate_c3 = remote(g_a.at[pl.ds(1, 1)], g_c.at[pl.ds(1, 1)], "C", "gate_c35", 2)
    gate_c5 = remote(g_b.at[pl.ds(1, 1)], g_c.at[pl.ds(2, 1)], "C", "gate_c35", 2)
    gate_c7 = remote(g_d.at[pl.ds(1, 1)], g_c.at[pl.ds(3, 1)], "C", "gate_c7", 2)

    await_all(lsem.at[1], gsend.at[pl.ds(0, 4)])
    ids_v, gates_v = ids[...], gates[...]
    for p, k in enumerate(GATE_ORDER):
        base = (me ^ k) * local_experts
        for e in range(local_experts):
            row = jnp.sum(jnp.where(ids_v == base + e, gates_v, 0.0), axis=0, keepdims=True)
            gsend[p, pl.ds(2 * e, 1), :] = row[:, :half]
            gsend[p, pl.ds(2 * e + 1, 1), :] = row[:, half:]
    await_all(lsem.at[0], xs.at[0])
    pl.semaphore_wait(barrier, 3)
    start(first[0])
    start((gate_a, gate_b))
    start(first[1])
    start((gate_c, core_own))
    start([pieces[0] for pieces in second[0]])

    def pass_first_0():
        arrive(("first", 0), xs.at[2, lower])
        start(onward[0])
        core[2].start()
        arrive("gate_ab", gsend.at[pl.ds(0, 6)])
        start((gate_c3, gate_c5, gate_d))

    def pass_first_1():
        arrive(("first", 1), xs.at[3, lower])
        start(onward[1])
        core[3].start()
        start([pieces[1] for pieces in second[0]])
        start([pieces[0] for pieces in second[1]])

    def pass_diagonal_0():
        arrive(("onward", 0), xs.at[4, lower])
        core[4].start()
        arrive("gate_d", g_d)
        gate_c7.start()

    def pass_diagonal_1():
        arrive(("onward", 1), xs.at[5, lower])
        core[5].start()

    def pass_second():
        arrive("second", xs.at[pl.ds(6, 2), lower])
        start((core[6], core[7]))

    gate_tiles = {
        0: gsend.at[0], 1: g_c.at[0], 2: g_a.at[0], 3: g_c.at[1],
        4: g_b.at[0], 5: g_c.at[2], 6: g_d.at[0], 7: g_c.at[3],
    }

    def hidden(s, part, e):
        tokens = xs[s, part]
        mask = jnp.concatenate([G[e, part]] * (w1.shape[2] // 128), axis=1) > 0.0
        a = jnp.dot(tokens, w1[e], preferred_element_type=F32)
        b = jnp.dot(tokens, w3[e], preferred_element_type=F32)
        return jnp.where(mask, a * (1.0 / (1.0 + jnp.exp(-a))) * b, 0.0).astype(BF16)

    def experts(s, total, finish, hooks=None, parts=(0, 1)):
        hooks = hooks or {}
        part = pl.ds(parts[0] * half, len(parts) * half)
        left = lax.broadcasted_iota(jnp.int32, (1, half), 1) < QUARTER
        for e in range(local_experts):
            for i in parts:
                (o0, h0, _), (o1, h1, _) = BLOCKS[s][2 * i:2 * i + 2]
                row = gate_tiles[o0][pl.ds(2 * e + h0, 1), :]
                if (o0, h0) != (o1, h1):
                    row = jnp.where(left, row, gate_tiles[o1][pl.ds(2 * e + h1, 1), :])
                G[e, pl.ds(i * half, half), :] = jnp.broadcast_to(row, (half, half)).T
        act = None
        for e in range(local_experts + 1):
            for hook in hooks.get(e, ()):
                hook()
            later = hidden(s, part, e) if e < local_experts else None
            if act is not None:
                out = jnp.dot(act, w2[e - 1], preferred_element_type=F32)
                out = out * jnp.concatenate([G[e - 1, part]] * (w2.shape[2] // 128), axis=1)
                if e == 1:
                    total[part, :] = out
                elif e < local_experts:
                    total[part, :] += out
                else:
                    finish(out)
            act = later

    back_c = {s: remote(out_c.at[s - 2], rec_c.at[s - 2], "C", ("back_c", s), 1) for s in range(2, 8)}
    back_own = [remote(out_c1.at[part], rec_c1.at[part], "C", "back_own", 1) for part in (upper, lower)]

    def finish_own(out):
        own[...] = own[...] + out

    def finish_core_own(part):
        def finish(out):
            out_c1[part, :] = (acc[0, part, :] + out).astype(BF16)
        return finish

    def finish_core(s):
        def finish(out):
            out_c[s - 2] = (acc[s % 2, upper, :] + out[:half]).astype(BF16)
        return finish

    def finish_chip(s):
        def finish(out):
            acc[s % 2, lower, :] += out[-half:]
        return finish

    held = []

    def send_chip(s):
        i = s - 2
        arrive(("back_c", s), rec_c.at[i])
        if s >= 6:
            arrive(("through", s - 2), d_ab.at[s - 6])
        for j, (owner, h, q) in enumerate(BLOCKS[s][2:]):
            part = pl.ds(j * QUARTER, QUARTER)
            total = acc[s % 2, pl.ds(half + j * QUARTER, QUARTER), :] + rec_c[i, part, :].astype(F32)
            if s >= 6:
                total = total + d_ab[s - 6, 1 if owner == 2 else 0].astype(F32)
            pb[i, part, :] = total.astype(BF16)
            row = pl.ds(token_row(h, q), QUARTER)
            if owner == 6:
                copy = remote(pb.at[i, part], d_ab.at[s - 4, h], "A" if h == 0 else "B", ("through", s), 1)
            elif s == 3:
                to, dst = ("A", r_a) if owner == 2 else ("B", r_b)
                rest, copy = (
                    remote(pb.at[i, pl.ds(j * QUARTER + skip, 32)], dst.at[pl.ds(token_row(h, q) + skip, 32)], to, "back", 1)
                    for skip in (32, 0)
                )
                held.append(rest)
            else:
                name = ("back", s) if s >= 6 else "back"
                to, dst = ("A", r_a.at[row]) if owner == 2 else ("B", r_b.at[row])
                copy = remote(pb.at[i, part], dst, to, name, 1)
            copy.start()
        if s == 4:
            start(held)

    def pair(s, *hooks):
        def finish(out):
            finish_core(s)(out)
            finish_chip(s)(out)
        if s < 7:
            arrive(("core", s), xs.at[s, upper] if s < 6 else xs.at[pl.ds(6, 2), upper])
        experts(s, acc.at[s % 2], finish, {2: hooks})
        back_c[s].start()

    do = functools.partial
    experts(0, own, finish_own, {e: [do(await_weights, e)] for e in range(local_experts)})
    pass_first_0()
    arrive("core_own", xs.at[1])
    arrive("gate_c", g_c.at[pl.ds(0, 1)])
    experts(1, acc.at[0], finish_core_own(upper), parts=(0,))
    back_own[0].start()
    arrive("gate_c35", g_c.at[pl.ds(1, 2)])
    pair(2, pass_first_1)
    pair(3, do(send_chip, 2), pass_diagonal_0)
    arrive("gate_c7", g_c.at[pl.ds(3, 1)])
    pair(4, do(send_chip, 3), pass_diagonal_1)
    pair(5, do(send_chip, 4), pass_second)
    pair(6, do(send_chip, 5))
    experts(7, acc.at[1], finish_core(7), {3: [do(send_chip, 6)]}, parts=(0,))
    back_c[7].start()
    experts(7, acc.at[1], finish_chip(7), parts=(1,))
    pl.when(x == 0)(do(send_chip, 7))
    experts(1, acc.at[0], finish_core_own(lower), {3: [do(pl.when(x == 1), do(send_chip, 7))]}, parts=(1,))
    back_own[1].start()

    own[...] = own[...] + xs[0].astype(F32)
    arrive("back", r_a)
    own[upper, :] = own[upper, :] + r_a[upper, :].astype(F32)
    own[lower, :] = own[lower, :] + r_b[lower, :].astype(F32)
    arrive("back_own", rec_c1)
    for s in (6, 7):
        arrive(("back", s), r_a.at[upper])
        for owner, h, q in BLOCKS[s][2:]:
            row = pl.ds(token_row(h, q), QUARTER)
            last = (r_a if owner == 2 else r_b)[row, :].astype(F32)
            y_ref[row, :] = (own[row, :] + rec_c1[row, :].astype(F32) + last).astype(BF16)
    await_all(ssem.at[0], xs.at[pl.ds(0, 7)])
    await_all(ssem.at[1], xs.at[pl.ds(0, 7)])
    await_all(ssem.at[2], G.at[0, pl.ds(0, 96)])


def solution(mesh):
    axes = tuple(mesh.axis_names)
    row_spec, w_spec = P(axes, None), P(axes, None, None)

    def local_layer(tokens, expert_ids, gate_weights, w_gate, w_up, w_down):
        rows, width = tokens.shape
        experts, _, ff = w_gate.shape
        top_k = expert_ids.shape[1]
        return pl.pallas_call(
            moe_kernel,
            name="moe_layer",
            out_shape=jax.ShapeDtypeStruct((rows, width), BF16),
            in_specs=[pl.BlockSpec(memory_space=pltpu.HBM)] * 6,
            out_specs=pl.BlockSpec(memory_space=pltpu.VMEM),
            scratch_shapes=[
                pltpu.VMEM((8, rows, width), BF16),
                pltpu.VMEM((experts, width, ff), BF16),
                pltpu.VMEM((experts, width, ff), BF16),
                pltpu.VMEM((experts, ff, width), BF16),
                pltpu.VMEM((top_k, rows), jnp.int32),
                pltpu.VMEM((top_k, rows), F32),
                pltpu.VMEM((8, 8, 128), F32),
                pltpu.VMEM((4, 8, 128), F32),
                pltpu.VMEM((2, 8, 128), F32),
                pltpu.VMEM((2, 8, 128), F32),
                pltpu.VMEM((4, 8, 128), F32),
                pltpu.VMEM((experts, rows, 128), F32),
                pltpu.VMEM((2, rows, width), F32),
                pltpu.VMEM((rows, width), F32),
                pltpu.VMEM((rows, width), BF16),
                pltpu.VMEM((rows, width), BF16),
                pltpu.VMEM((6, rows // 2, width), BF16),
                pltpu.VMEM((6, rows // 2, width), BF16),
                pltpu.VMEM((6, rows // 2, width), BF16),
                pltpu.VMEM((rows, width), BF16),
                pltpu.VMEM((rows, width), BF16),
                pltpu.VMEM((2, 2, QUARTER, width), BF16),
                pltpu.SemaphoreType.DMA((6,)),
                pltpu.SemaphoreType.DMA((3,)),
                pltpu.SemaphoreType.DMA((28,)),
            ],
            compiler_params=pltpu.CompilerParams(
                collective_id=0, has_side_effects=True, vmem_limit_bytes=46 * 2**20
            ),
        )(*(pltpu.with_memory_space_constraint(v, pltpu.HBM) for v in (tokens, expert_ids.T, gate_weights.T, w_gate, w_up, w_down)))

    return jax.shard_map(
        local_layer, mesh=mesh,
        in_specs=(row_spec, row_spec, row_spec, w_spec, w_spec, w_spec),
        out_specs=row_spec, check_vma=False,
    )
```
